256 devices in a mesh: gx: 8 (over z_lo, core), gy: 4 (over y), gz: 8 (over z_hi, x).
Axes of the slice: x: 4, y: 4, z: 8 (z_hi: 2, z_lo: 4; z = z_hi * 4 + z_lo), core: 2. Of those that a mesh axis runs over, the one named last changes fastest.
Arguments:
- raw_weight: float32 [128, 27, 128], P(('gx', 'gy')), may hold values from -6 to 6
- inputs: bfloat16 [64, 64, 128, 128], P('gx', 'gy', 'gz'), may hold values from -6 to 6
- cotangent: bfloat16 [64, 64, 128, 128], P('gx', 'gy', 'gz'), may hold values from -0.099609375 to 0.099609375
Outputs:
- input_grad: bfloat16 [64, 64, 128, 128], P('gx', 'gy', 'gz')
- weight_grad: float32 [128, 27, 128], P(('gx', 'gy'))
The draws below stay inside these ranges and needn't reach their ends.
All inputs are finite; a program needn't handle non-finite values.
Results may differ from the reference program's by a relative error of at most 0.0049.
Values may be sent and summed in bfloat16 or wider, within the bound.
A program may use at most 64 MiB of HBM per device.

```python
import math
import jax
import jax.numpy as jnp
from jax import lax

C = 128
KK = 27
NX = 64
NY = 64
NZ = 128


def draw_raw_weight(key, part):
    sub_keys = jax.random.split(key, 4)
    row_scale = jnp.exp(jax.random.uniform(sub_keys[0], (C, 1, 1), jnp.float32, math.log(0.1), 0.0))
    col_scale = jnp.exp(jax.random.uniform(sub_keys[1], (1, 1, C), jnp.float32, math.log(0.1), 0.0))
    col_mean = jax.random.uniform(sub_keys[2], (1, 1, C), jnp.float32, -0.5, 0.5)
    base_draw = jnp.clip(jax.random.normal(sub_keys[3], (C, KK, C), jnp.float32), -4.0, 4.0)
    return jnp.clip((base_draw * row_scale + col_mean) * col_scale, -6.0, 6.0)


def steps_of(rng, shape, cuts, smallest, top_value):
    def one(dim, parts):
        steps = jax.random.uniform(jax.random.fold_in(jax.random.fold_in(rng, 6), dim), (parts,), jnp.float32, smallest / len(cuts), top_value / len(cuts))
        return jnp.repeat(jnp.exp(steps), shape[dim] // parts).reshape((-1,) + (1,) * (len(shape) - dim - 1))

    level = one(*cuts[0])
    for cut in cuts[1:]:
        level = level * one(*cut)
    return level


def normal_values(rng, shape, scale, most, shards=(), dtype=jnp.bfloat16):
    array = jax.random.normal(rng, shape, jnp.float32) * scale
    if len(shards) > 0:
        array = steps_of(rng, shape, shards, -0.22, 0.18) * array
    return jnp.clip(array, min=-most, max=most).astype(dtype)


def setup_inputs(seed: int = 0) -> dict:
    key_of = jax.random.split(jax.random.key(seed), 4)
    raw_weight = draw_raw_weight(jax.random.fold_in(key_of[3], 71), 0)
    inputs = normal_values(key_of[1], (NX, NY, NZ, C), 1.0, 6.0, ((0, 8), (1, 4), (2, 8)))
    cotangent = normal_values(key_of[2], (NX, NY, NZ, C), 0.017, 0.099609375, ((0, 8), (1, 4), (2, 8)))
    return dict(raw_weight=raw_weight, inputs=inputs, cotangent=cotangent)


var_eps = 1e-05
norm_eps = 1e-06
clip_norm = 600.0

def tap_view(padded, tap_a, tap_b, tap_c, extent):
    view = padded[2 - tap_a:2 - tap_a + extent[0], 2 - tap_b:2 - tap_b + extent[1], 2 - tap_c:2 - tap_c + extent[2], :]
    return view.reshape(-1, view.shape[-1])

def reference(raw_weight, inputs, cotangent):
    extent = inputs.shape[:3]
    channels = inputs.shape[3]
    fan_count = raw_weight.shape[0] * raw_weight.shape[1]
    sum_first = lax.optimization_barrier(jnp.sum(raw_weight, axis=(0, 1)))
    sum_second = lax.optimization_barrier(jnp.sum(raw_weight * raw_weight, axis=(0, 1)))
    mean_out = sum_first / fan_count
    var_out = sum_second / fan_count - mean_out * mean_out
    inv_std = lax.rsqrt(var_out + var_eps)
    std_float = (raw_weight - mean_out) * inv_std
    std_half = lax.optimization_barrier(std_float.astype(jnp.bfloat16)).astype(jnp.float32)
    padded = jnp.pad(cotangent.astype(jnp.float32), ((1, 1), (1, 1), (1, 1), (0, 0)))
    flat_in = inputs.astype(jnp.float32).reshape(-1, channels)
    dx_total = jnp.zeros((flat_in.shape[0], channels), jnp.float32)
    pieces = []
    for tap_a in range(3):
        for tap_b in range(3):
            for tap_c in range(3):
                tap_index = tap_a * 9 + tap_b * 3 + tap_c
                view = tap_view(padded, tap_a, tap_b, tap_c, extent)
                dx_total = dx_total + jnp.dot(view, std_half[:, tap_index, :].T, precision=lax.Precision.HIGHEST)
                pieces.append(jnp.dot(flat_in.T, view, precision=lax.Precision.HIGHEST))
    input_grad = dx_total.reshape(extent[0], extent[1], extent[2], channels).astype(jnp.bfloat16)
    filter_grad = jnp.stack(pieces, axis=1)
    mean_grad = lax.optimization_barrier(jnp.sum(filter_grad, axis=(0, 1))) / fan_count
    mean_cross = lax.optimization_barrier(jnp.sum(filter_grad * std_float, axis=(0, 1))) / fan_count
    raw_grad = inv_std * (filter_grad - mean_grad - std_float * mean_cross)
    square_sum = jnp.sum(raw_grad * raw_grad)
    scale = jnp.minimum(1.0, clip_norm * lax.rsqrt(square_sum + norm_eps))
    return (input_grad, raw_grad * scale)
```

```python
import functools

import jax
import jax.numpy as jnp
from jax import lax
from jax.experimental import pallas as pl
from jax.experimental.pallas import tpu as pltpu
from jax.sharding import PartitionSpec as P

var_eps = 1e-05
norm_eps = 1e-06
clip_norm = 600.0

f32 = jnp.float32
bf16 = jnp.bfloat16
MESH = pl.DeviceIdType.MESH

C = 128
LX, LY, LZ = 8, 16, 16
CELLS = LX * LY * LZ
PITCH = 32
FAN = 27 * C

TAPS = [(ab // 3, ab % 3, c) for c in (1, 0, 2) for ab in range(9)]
WIDTH_TAPS = (1, 0, 2)
CHUNKS = ((0, 2), (2, 5), (5, 7))
DIRECTIONS = [
    (dx, dy, dz)
    for dz in (-1, 1, 0)
    for dx in (0, -1, 1)
    for dy in (0, -1, 1)
    if (dx, dy, dz) != (0, 0, 0)
]


def body(raw_ref, x_ref, cot_ref, dx_ref, dw_ref, full, pad, zface, zedge, zhalo, zcorner, xt,
         rawp, raws, part, w, own, psend, precv, spread, r1, red, r2, rows, gath, nat, stat,
         hs, hr, ws, wr, fs, fr, ds, dr, s1, q1, s2, q2, s3, q3, s4, q4):
    gx, gy, gz = lax.axis_index("gx"), lax.axis_index("gy"), lax.axis_index("gz")
    z_lo, core = gx // 2, gx % 2
    z_hi, x = gz // 4, gz % 4
    z = z_hi * 4 + z_lo
    mine = gy * 4 + x
    full2 = full.reshape(10 * 18 * PITCH, C)

    def dev(a, b, c):
        return (a, b, c)

    def gx_peer(k):
        return dev((gx + k) % 8, gy, gz)

    def chip_peer(k):
        return dev(((z_lo + k) % 4) * 2 + core, gy, gz)

    def gy_peer(k):
        return dev(gx, (gy + k) % 4, gz)

    def x_peer(k):
        return dev(gx, gy, z_hi * 4 + (x + k) % 4)

    def xy_peer(k):
        return dev(gx, (gy + k // 4) % 4, z_hi * 4 + (x + k % 4) % 4)

    def z_peer(k):
        zz = (z + k) % 8
        return dev((zz % 4) * 2 + core, gy, (zz // 4) * 4 + x)

    def plane_peer(k):
        return dev((gx + k // 4) % 8, (gy + k % 4) % 4, gz)

    partner = dev(gx + 1 - 2 * core, gy, gz)

    def remote(src, dst, send, recv, device):
        return pltpu.make_async_remote_copy(
            src_ref=src, dst_ref=dst, send_sem=send, recv_sem=recv, device_id=device, device_id_type=MESH
        )

    def drain(ref, sem):
        pltpu.make_async_copy(ref, ref, sem).wait()

    def exists(axis_index, last, step):
        if step == 0:
            return None
        return axis_index > 0 if step < 0 else axis_index < last

    def present(d):
        tests = [exists(gx, 7, d[0]), exists(gy, 3, d[1]), exists(gz, 7, d[2])]
        tests = [t for t in tests if t is not None]
        out = tests[0]
        for t in tests[1:]:
            out = jnp.logical_and(out, t)
        return out

    barrier = pltpu.get_barrier_semaphore()

    def greet(device):
        pl.semaphore_signal(barrier, inc=1, device_id=device, device_id_type=MESH)

    wide = [d for d in DIRECTIONS if d[2] != 0]
    greeted = jnp.int32(0)
    for d in wide:
        there = present(d)

        @pl.when(there)
        def _(d=d):
            greet(dev(gx + d[0], gy + d[1], gz + d[2]))

        greeted = greeted + there.astype(jnp.int32)
    lax.fori_loop(1, 8, lambda k, _: (greet(z_peer(k)), 0)[1], 0)
    lax.fori_loop(1, 16, lambda k, _: (greet(xy_peer(k)), 0)[1], 0)
    lax.fori_loop(1, 32, lambda k, _: (greet(plane_peer(k)), 0)[1], 0)

    def fill(i, _):
        slab = cot_ref[i]
        pad[1, i + 1, 1 : LY + 1] = slab
        full[i + 1, 1 : LY + 1, 8 : 8 + LZ, :] = slab.astype(f32)
        return 0

    lax.fori_loop(0, LX, fill, 0)

    def faces(i, _):
        for s, zr in ((0, 8), (1, 8 + LZ - 1)):
            zface[s, i] = full2[pl.ds(((i + 1) * 18 + 1) * PITCH + zr, LY, stride=PITCH), :].astype(bf16)
        return 0

    lax.fori_loop(0, LX, faces, 0)
    for s, zr in ((0, 8), (1, 8 + LZ - 1)):
        for e, yr in ((0, 1), (1, LY)):
            for i in range(LX):
                at = ((i + 1) * 18 + yr) * PITCH + zr
                zedge[s, e, i : i + 1, :] = full2[at : at + 1, :]
    for r in range(4):
        rawp[r * 32 : r * 32 + 27, :] = raw_ref[r]
        rawp[r * 32 + 27 : r * 32 + 32, :] = jnp.zeros((5, C), f32)
    raws[gy] = rawp[...]

    tile = jnp.zeros((LZ, C), bf16)

    @pl.when(gx == 0)
    def _():
        for j in range(18):
            pad[1, 0, j] = tile

    @pl.when(gx == 7)
    def _():
        for j in range(18):
            pad[1, 9, j] = tile

    @pl.when(gy == 0)
    def _():
        for i in range(10):
            pad[1, i, 0] = tile

    @pl.when(gy == 3)
    def _():
        for i in range(10):
            pad[1, i, 17] = tile

    for s, gone in ((0, gz == 0), (1, gz == 7)):

        @pl.when(gone)
        def _(s=s):
            for i in range(10):
                zhalo[s, i] = tile
            for e in range(2):
                for k in range(3):
                    zcorner[s, e, k] = jnp.zeros((8, C), f32)

        @pl.when(jnp.logical_and(jnp.logical_not(gone), gx == 0))
        def _(s=s):
            zhalo[s, 0] = tile
            for e in range(2):
                zcorner[s, e, 0] = jnp.zeros((8, C), f32)

        @pl.when(jnp.logical_and(jnp.logical_not(gone), gx == 7))
        def _(s=s):
            zhalo[s, 9] = tile
            for e in range(2):
                zcorner[s, e, 2] = jnp.zeros((8, C), f32)

        for e, lost in ((0, gy == 0), (1, gy == 3)):

            @pl.when(jnp.logical_and(jnp.logical_not(gone), lost))
            def _(s=s, e=e):
                for k in range(3):
                    zcorner[s, e, k] = jnp.zeros((8, C), f32)

    pl.semaphore_wait(barrier, greeted + (7 + 15 + 31))

    def halo_copy(n, d):
        dx, dy, dz = d
        xs, xd = (None, None) if dx == 0 else ((0, 9) if dx < 0 else (LX - 1, 0))
        ys, yd = (None, None) if dy == 0 else ((0, 17) if dy < 0 else (LY - 1, 0))
        if dz == 0:
            if dy == 0:
                src, dst = cot_ref.at[xs], pad.at[1, xd, pl.ds(1, LY)]
            elif dx == 0:
                src, dst = cot_ref.at[:, ys], pad.at[1, pl.ds(1, LX), yd]
            else:
                src, dst = cot_ref.at[xs, ys], pad.at[1, xd, yd]
        else:
            s = 0 if dz < 0 else 1
            r = 1 - s
            if dy == 0:
                if dx == 0:
                    src, dst = zface.at[s], zhalo.at[r, pl.ds(1, LX)]
                else:
                    src, dst = zface.at[s, xs], zhalo.at[r, xd]
            else:
                e = 0 if dy < 0 else 1
                k = 1 if dx == 0 else (2 if dx < 0 else 0)
                src, dst = zedge.at[s, e], zcorner.at[r, 1 - e, k]
        return remote(src, dst, hs.at[n], hr.at[n], dev(gx + dx, gy + dy, gz + dz))

    for n, d in enumerate(DIRECTIONS):

        @pl.when(present(d))
        def _(n=n, d=d):
            halo_copy(n, d).start()

    def halo_wait(flat):
        for n, d in enumerate(DIRECTIONS):
            if (d[2] == 0) == flat:

                @pl.when(present((-d[0], -d[1], -d[2])))
                def _(n=n, d=d):
                    halo_copy(n, d).wait_recv()

    def to_gy(k, _):
        remote(rawp, raws.at[gy], ws.at[0], wr.at[0], gy_peer(k)).start()
        return 0

    lax.fori_loop(1, 4, to_gy, 0)

    m = lax.broadcasted_iota(jnp.int32, (C, C), 0)
    col = lax.broadcasted_iota(jnp.int32, (C, C), 1)
    want = (m % 4) * 32 + (m // 4 + 16 * core) % 32
    order = jnp.where(col == want, 1.0, 0.0).astype(bf16)
    for j in range(4):
        xt[:, j * 512 : (j + 1) * 512] = lax.dot_general(
            order,
            x_ref[2 * j : 2 * j + 2].reshape(512, C),
            (((1,), (1,)), ((), ())),
            preferred_element_type=f32,
        ).astype(bf16)

    drain(raws.at[pl.ds(0, 3)], wr.at[0])
    first = jnp.zeros((1, C), f32)
    second = jnp.zeros((1, C), f32)
    for j in range(4):
        v = raws[j]
        first = first + jnp.sum(v, axis=0, keepdims=True)
        second = second + jnp.sum(v * v, axis=0, keepdims=True)
    row = lax.broadcasted_iota(jnp.int32, (8, C), 0)
    part[gx] = jnp.where(row == 0, first, jnp.where(row == 1, second, 0.0))

    def to_gx(k, _):
        remote(part.at[gx], part.at[gx], ws.at[1], wr.at[1], gx_peer(k)).start()
        return 0

    lax.fori_loop(1, 8, to_gx, 0)

    def quad(q):
        outs = []
        for h in range(2):
            views = []
            for p in (4 * q + 2 * h, 4 * q + 2 * h + 1):
                if p < 27:
                    a, b, c = TAPS[p]
                    views.append(pad[c, 2 - a : 2 - a + LX, 2 - b : 2 - b + LY].reshape(CELLS, C))
            v = jnp.concatenate(views, axis=1) if len(views) == 2 else views[0]
            o = jnp.dot(xt[...], v, preferred_element_type=f32)
            outs.append(o[:, :C])
            outs.append(o[:, C:] if len(views) == 2 else jnp.zeros((C, C), f32))
        low = lax.broadcasted_iota(jnp.int32, (16, 8, C), 1) < 4
        pieces = [[], []]
        for h in range(2):
            one = outs[2 * h].reshape(16, 8, C)
            two = outs[2 * h + 1].reshape(16, 8, C)
            pieces[0].append(jnp.where(low, one, pltpu.roll(two, 4, 1)))
            pieces[1].append(jnp.where(low, pltpu.roll(one, 4, 1), two))
        for e in range(2):
            t = jnp.concatenate(pieces[e], axis=1)
            for j in range(8):
                own[q, 2 * j + e] = t[j]
                psend[q, 2 * j + e] = t[8 + j].astype(bf16)
        remote(psend.at[q], precv.at[q], ds.at[q], dr.at[q], partner).start()

    def spread_chunk(n):
        lo, hi = CHUNKS[n]
        for q in range(lo, hi):
            drain(precv.at[q], dr.at[q])

            def mix(d, _, q=q):
                spread[d, q] = (own[q, d] + precv[q, d].astype(f32)).astype(bf16)
                return 0

            lax.fori_loop(0, 16, mix, 0, unroll=4)

        def send(k, _):
            there = ((gy + k // 4) % 4) * 4 + (x + k % 4) % 4
            remote(
                spread.at[there, pl.ds(lo, hi - lo)],
                r1.at[k - 1, pl.ds(lo, hi - lo)],
                s1.at[n],
                q1.at[n],
                xy_peer(k),
            ).start()
            return 0

        lax.fori_loop(1, 16, send, 0)

    halo_wait(True)
    quad(0)
    quad(1)

    drain(part.at[pl.ds(0, 7)], wr.at[1])
    total = part[0]
    for j in range(1, 8):
        total = total + part[j]
    mean = total[0:1] / FAN
    var = total[1:2] / FAN - mean * mean
    inv = lax.rsqrt(var + var_eps)
    raws2 = raws.reshape(512, C)
    mine_rows = pl.ds(pl.multiple_of(gx * 16, 16), 16)
    for p in range(27):
        a, b, c = TAPS[p]
        t = 9 * a + 3 * b + c
        v = raws2[pl.ds(t, 16, stride=32), :]
        w[mine_rows, p * C : (p + 1) * C] = ((v - mean) * inv).astype(bf16)

    def slab(g):
        return w.at[pl.ds(pl.multiple_of(g * 16, 16), 16)]

    def to_z(k, _):
        remote(slab(gx), slab(gx), ws.at[2], wr.at[2], chip_peer(k)).start()
        return 0

    lax.fori_loop(1, 4, to_z, 0)
    remote(slab(gx), slab(gx), fs.at[0], fr.at[0], partner).start()

    for i in (0, 9):
        full[i, :, 8 : 8 + LZ, :] = pad[1, i].astype(f32)
    for j in (0, 17):
        full[1 : LX + 1, j, 8 : 8 + LZ, :] = pad[1, 1 : LX + 1, j].astype(f32)
    spread_chunk(0)
    halo_wait(False)
    for s, zr in ((0, 7), (1, 8 + LZ)):

        def put(i, _, s=s, zr=zr):
            full2[pl.ds((i * 18 + 1) * PITCH + zr, LY, stride=PITCH), :] = zhalo[s, i].astype(f32)
            return 0

        lax.fori_loop(0, 10, put, 0)
        for e, yr in ((0, 0), (1, 17)):
            for i in range(10):
                at = (i * 18 + yr) * PITCH + zr
                k, r = (1, i - 1) if 0 < i < 9 else ((0, 7) if i == 0 else (2, 0))
                full2[at : at + 1, :] = zcorner[s, e, k, r : r + 1, :]

    def shift(i, _):
        pad[0, i] = full[i, :, 9 : 9 + LZ, :].astype(bf16)
        pad[2, i] = full[i, :, 7 : 7 + LZ, :].astype(bf16)
        return 0

    lax.fori_loop(0, 10, shift, 0)
    for q in range(2, 5):
        quad(q)
    quad(5)
    spread_chunk(1)
    quad(6)

    drain(w.at[pl.ds(0, 48)], wr.at[2])
    spread_chunk(2)

    def hand_on(k, _):
        g = ((z_lo + k) % 4) * 2 + core
        remote(slab(g), slab(g), fs.at[1], fr.at[1], partner).start()
        return 0

    lax.fori_loop(1, 4, hand_on, 0)

    def input_grad(i0, count):
        def one(i, _):
            views = []
            for a, b, c in TAPS:
                v = pad[c, pl.ds(2 * i + 2 - a, 2), 2 - b : 2 - b + LY]
                views.append(v.reshape(2 * LY * LZ, C))
            out = lax.dot_general(
                jnp.concatenate(views, axis=1), w[...], (((1,), (1,)), ((), ())), preferred_element_type=f32
            )
            dx_ref[pl.ds(2 * i, 2)] = out.astype(bf16).reshape(2, LY, LZ, C)
            return 0

        lax.fori_loop(i0, i0 + count, one, 0)

    for n in range(3):
        lo, hi = CHUNKS[n]
        drain(r1.at[:, pl.ds(lo, hi - lo)], q1.at[n])
    for q in range(7):
        acc = own[q, mine] + precv[q, mine].astype(f32)
        for k in range(15):
            acc = acc + r1[k, q].astype(f32)
        red[q * 16 : (q + 1) * 16, :] = acc
    red[112:128, :] = jnp.zeros((16, C), f32)
    for j in range(4):
        rows[j] = red[pl.ds(j, 32, stride=4), :].astype(bf16)
    r2[z] = rows[z_lo]

    def to_all_z(k, _):
        remote(rows.at[(z_lo + k) % 4], r2.at[z], s2.at[0], q2.at[0], z_peer(k)).start()
        return 0

    lax.fori_loop(1, 8, to_all_z, 0)

    drain(w.at[pl.ds(0, 16)], fr.at[0])
    drain(w.at[pl.ds(0, 48)], fr.at[1])
    input_grad(0, 2)

    drain(r2.at[pl.ds(0, 7)], q2.at[0])
    acc = r2[0].astype(f32)
    for j in range(1, 8):
        acc = acc + r2[j].astype(f32)
    gath[x] = acc

    def to_x(k, _):
        remote(gath.at[x], gath.at[x], s3.at[0], q3.at[0], x_peer(k)).start()
        return 0

    lax.fori_loop(1, 4, to_x, 0)
    input_grad(2, 1)

    drain(gath.at[pl.ds(0, 3)], q3.at[0])
    for r in range(4):
        for n, c in enumerate(WIDTH_TAPS):
            nat[pl.ds(r * 32 + c, 9, stride=3), :] = gath[r, n * 9 : n * 9 + 9, :]
    g_first = jnp.zeros((1, C), f32)
    g_cross = jnp.zeros((1, C), f32)
    g_second = jnp.zeros((1, C), f32)
    for r in range(4):
        g = nat[r * 32 : r * 32 + 27, :]
        std = (raw_ref[r] - mean) * inv
        g_first = g_first + jnp.sum(g, axis=0, keepdims=True)
        g_cross = g_cross + jnp.sum(g * std, axis=0, keepdims=True)
        g_second = g_second + jnp.sum(g * g, axis=0, keepdims=True)
    stat[gx * 4 + gy] = jnp.where(
        row == 0, g_first, jnp.where(row == 1, g_cross, jnp.where(row == 2, g_second, 0.0))
    )

    def to_plane(k, _):
        here = stat.at[gx * 4 + gy]
        remote(here, here, s4.at[0], q4.at[0], plane_peer(k)).start()
        return 0

    lax.fori_loop(1, 32, to_plane, 0)
    input_grad(3, 1)
    drain(stat.at[pl.ds(0, 31)], q4.at[0])
    total = stat[0]
    for j in range(1, 32):
        total = total + stat[j]
    sum_grad, sum_cross, sum_square = total[0:1], total[1:2], total[2:3]
    mean_grad = sum_grad / FAN
    mean_cross = sum_cross / FAN
    per_output = sum_square - 2.0 * mean_grad * sum_grad - 2.0 * mean_cross * sum_cross
    per_output = (
        per_output + FAN * mean_grad * mean_grad + FAN * mean_cross * mean_cross * var / (var + var_eps)
    )
    square_sum = jnp.sum(inv * inv * per_output, axis=1, keepdims=True)
    scale = jnp.minimum(1.0, clip_norm * lax.rsqrt(square_sum + norm_eps))
    for r in range(4):
        g = nat[r * 32 : r * 32 + 27, :]
        std = (raw_ref[r] - mean) * inv
        dw_ref[r] = inv * (g - mean_grad - std * mean_cross) * scale

    for n, d in enumerate(DIRECTIONS):

        @pl.when(present(d))
        def _(n=n, d=d):
            halo_copy(n, d).wait_send()

    drain(raws.at[pl.ds(0, 3)], ws.at[0])
    drain(part.at[pl.ds(0, 7)], ws.at[1])
    drain(w.at[pl.ds(0, 48)], ws.at[2])
    drain(w.at[pl.ds(0, 16)], fs.at[0])
    drain(w.at[pl.ds(0, 48)], fs.at[1])
    for q in range(7):
        drain(precv.at[q], ds.at[q])
    for n in range(3):
        lo, hi = CHUNKS[n]
        drain(r1.at[:, pl.ds(lo, hi - lo)], s1.at[n])
    drain(r2.at[pl.ds(0, 7)], s2.at[0])
    drain(gath.at[pl.ds(0, 3)], s3.at[0])
    drain(stat.at[pl.ds(0, 31)], s4.at[0])


def on_device(raw_weight, inputs, cotangent):
    dma = pltpu.SemaphoreType.DMA
    vmem = pltpu.VMEM
    return pl.pallas_call(
        body,
        out_shape=(
            jax.ShapeDtypeStruct(inputs.shape, bf16),
            jax.ShapeDtypeStruct(raw_weight.shape, f32),
        ),
        in_specs=[pl.BlockSpec(memory_space=pltpu.VMEM)] * 3,
        out_specs=[pl.BlockSpec(memory_space=pltpu.VMEM)] * 2,
        scratch_shapes=[
            vmem((10, 18, PITCH, C), f32),
            vmem((3, 10, 18, LZ, C), bf16),
            vmem((2, LX, LY, C), bf16),
            vmem((2, 2, 8, C), f32),
            vmem((2, 10, LY, C), bf16),
            vmem((2, 2, 3, 8, C), f32),
            vmem((C, CELLS), bf16),
            vmem((128, C), f32),
            vmem((4, 128, C), f32),
            vmem((8, 8, C), f32),
            vmem((C, 27 * C), bf16),
            vmem((7, 16, 16, C), f32),
            vmem((7, 16, 16, C), bf16),
            vmem((7, 16, 16, C), bf16),
            vmem((16, 7, 16, C), bf16),
            vmem((15, 7, 16, C), bf16),
            vmem((128, C), f32),
            vmem((8, 32, C), bf16),
            vmem((4, 32, C), bf16),
            vmem((4, 32, C), f32),
            vmem((128, C), f32),
            vmem((32, 8, C), f32),
            dma((26,)), dma((26,)),
            dma((3,)), dma((3,)),
            dma((2,)), dma((2,)),
            dma((7,)), dma((7,)),
            dma((3,)), dma((3,)),
            dma((1,)), dma((1,)),
            dma((1,)), dma((1,)),
            dma((1,)), dma((1,)),
        ],
        compiler_params=pltpu.CompilerParams(
            collective_id=0, has_side_effects=True, vmem_limit_bytes=40 * 1024 * 1024
        ),
    )(raw_weight, inputs, cotangent)


def solution(mesh):
    in_specs = (P(("gx", "gy"), None, None), P("gx", "gy", "gz", None), P("gx", "gy", "gz", None))
    out_specs = (P("gx", "gy", "gz", None), P(("gx", "gy"), None, None))
    return jax.shard_map(
        on_device, mesh=mesh, in_specs=in_specs, out_specs=out_specs, check_vma=False
    )
```

```python
import functools

import jax
import jax.numpy as jnp
from jax import lax
from jax.experimental import pallas as pl
from jax.experimental.pallas import tpu as pltpu
from jax.sharding import PartitionSpec as P

var_eps = 1e-05
norm_eps = 1e-06
clip_norm = 600.0

f32 = jnp.float32
bf16 = jnp.bfloat16
MESH = pl.DeviceIdType.MESH

C = 128
LX, LY, LZ = 8, 16, 16
CELLS = LX * LY * LZ
PITCH = 32
FAN = 27 * C

TAPS = [(t // 9, t // 3 % 3, t % 3) for t in range(27)]
CHUNKS = ((0, 2), (2, 4), (4, 7))
DIRECTIONS = [
    (dx, dy, dz)
    for dz in (-1, 1, 0)
    for dx in (0, -1, 1)
    for dy in (0, -1, 1)
    if (dx, dy, dz) != (0, 0, 0)
]


def body(raw_hbm, x_hbm, cot_hbm, dx_ref, dw_ref, raw_ref, x_ref, cot_ref,
         full, pad, zface, zedge, zpoint, zhalo, zcorner, zdot, plane, turned, xf, xt, xz, base,
         raws, mine_raw, part, w, wt, part_dx, own, psend, precv, spread, r1, red, comp, r2, rows, gath, nat, mine_std, stat,
         ls, hr, wr, dr, ours, got, sent):
    gx, gy, gz = lax.axis_index("gx"), lax.axis_index("gy"), lax.axis_index("gz")
    def div(a, n):
        return lax.div(a, jnp.int32(n))

    def mod(a, n):
        return lax.rem(a, jnp.int32(n))

    z_lo, core = div(gx, 2), mod(gx, 2)
    z_hi, x = div(gz, 4), mod(gz, 4)
    z = z_hi * 4 + z_lo
    mine = gy * 4 + x
    early_tap, late_tap = 2 - 2 * z_hi, 2 * z_hi
    early_side, late_side = z_hi, 1 - z_hi
    full2 = full.reshape(10 * 18 * PITCH, C)

    def dev(a, b, c):
        return (a, b, c)

    def ring(step):
        zz = mod(z + step, 8)
        return mod(zz, 4), div(zz, 4)

    spots = [ring(step) for step in range(8)] + [ring(2 + 4 * core)]
    at_gz = [hi * 4 + x for _, hi in spots]
    at_gx = [[lo * 2 + core, lo * 2 + 1 - core] for lo, _ in spots]
    at_gy = [gy] + [mod(gy + k, 4) for k in range(1, 4)]
    at_x = [x] + [mod(x + k, 4) for k in range(1, 4)]
    x_gz = [gz] + [z_hi * 4 + at_x[k] for k in range(1, 4)]

    def chip_peer(step):
        return dev(at_gx[step][0], gy, at_gz[step])

    def gy_peer(k):
        return dev(gx, at_gy[k], gz)

    def x_peer(k):
        return dev(gx, gy, x_gz[k])

    def xy_peer(k):
        return dev(gx, at_gy[k // 4], x_gz[k % 4])

    z_peer = chip_peer
    def plane_peer(k, step):
        return dev(at_gx[step][k // 4], at_gy[k % 4], at_gz[step])

    def to_plane(send, steps=(2, 1, 7, 0)):
        for step in steps:
            for k in range(1 if step == 0 else 0, 8):
                send(plane_peer(k, step))

    partner = dev(gx + 1 - 2 * core, gy, gz)

    def remote(src, dst, recv, device):
        return pltpu.make_async_remote_copy(
            src_ref=src, dst_ref=dst, send_sem=sent.at[0], recv_sem=recv, device_id=device, device_id_type=MESH
        )

    def rows_wait(n, sem):
        view = full2.at[pl.ds(0, n)]
        pltpu.make_async_copy(view, view, sem).wait()

    def drain(ref, sem):
        pltpu.make_async_copy(ref, ref, sem).wait()

    def exists(axis_index, last, step):
        if step == 0:
            return None
        return axis_index > 0 if step < 0 else axis_index < last

    def count(axis_index, last):
        return (axis_index > 0).astype(jnp.int32) + (axis_index < last).astype(jnp.int32)

    def present(d):
        tests = [exists(gx, 7, d[0]), exists(gy, 3, d[1]), exists(gz, 7, d[2])]
        tests = [t for t in tests if t is not None]
        out = tests[0]
        for t in tests[1:]:
            out = jnp.logical_and(out, t)
        return out

    loads = [
        pltpu.make_async_copy(a, b, ls.at[n])
        for n, (a, b) in enumerate(((cot_hbm, cot_ref), (raw_hbm, raw_ref), (x_hbm, x_ref)))
    ]
    for load in loads:
        load.start()

    barrier = pltpu.get_barrier_semaphore()

    def greet(device):
        pl.semaphore_signal(barrier, inc=1, device_id=device, device_id_type=MESH)

    wide = [d for d in DIRECTIONS if d[2] != 0]
    greeted = jnp.int32(0)
    for d in wide:
        there = present(d)

        @pl.when(there)
        def _(d=d):
            greet(dev(gx + d[0], gy + d[1], gz + d[2]))

        greeted = greeted + there.astype(jnp.int32)
    for k in (4, 3, 5, 2):
        greet(z_peer(k))
    for k in (10, 11, 9, 6, 14, 5, 7, 13, 15, 1, 2, 3):
        greet(xy_peer(k))
    to_plane(greet, (6, 1, 7, 0))

    loads[0].wait()

    def fill(i, _):
        slab = cot_ref[i]
        pad[1, i + 1, 1 : LY + 1] = slab
        full[i + 1, 1 : LY + 1, 8 : 8 + LZ, :] = slab.astype(f32)
        return 0

    lax.fori_loop(0, LX, fill, 0)

    def faces(i, _):
        for s, zr in ((0, 8), (1, 8 + LZ - 1)):
            zface[s, i] = full2[pl.ds(((i + 1) * 18 + 1) * PITCH + zr, LY, stride=PITCH), :].astype(bf16)
        return 0

    lax.fori_loop(0, LX, faces, 0)
    for s, zr in ((0, 8), (1, 8 + LZ - 1)):
        for e, yr in ((0, 1), (1, LY)):
            for i in range(LX):
                at = ((i + 1) * 18 + yr) * PITCH + zr
                zedge[s, e, i : i + 1, :] = full2[at : at + 1, :]
            zpoint[s, e, 0] = zedge[s, e, 0:1, :]
            zpoint[s, e, 1] = zedge[s, e, LX - 1 : LX, :]
    for i in range(10):
        for zr in (7, 8 + LZ):
            full2[pl.ds(i * 18 * PITCH + zr, 18, stride=PITCH), :] = jnp.zeros((18, C), f32)
    loads[1].wait()
    raws[gy] = raw_ref[...]
    first = jnp.zeros((4, C), f32)
    second = jnp.zeros((4, C), f32)
    for t in range(27):
        v = raw_ref[t]
        first = first + v
        second = second + v * v
    part[gx * 4 + gy, 0:1, :] = jnp.sum(first, axis=0, keepdims=True)
    part[gx * 4 + gy, 1:2, :] = jnp.sum(second, axis=0, keepdims=True)

    tile = jnp.zeros((LZ, C), bf16)

    @pl.when(gx == 0)
    def _():
        for j in range(18):
            pad[1, 0, j] = tile

    @pl.when(gx == 7)
    def _():
        for j in range(18):
            pad[1, 9, j] = tile

    @pl.when(gy == 0)
    def _():
        for i in range(10):
            pad[1, i, 0] = tile

    @pl.when(gy == 3)
    def _():
        for i in range(10):
            pad[1, i, 17] = tile

    for r, z_there in ((0, gz > 0), (1, gz < 7)):

        @pl.when(jnp.logical_not(z_there))
        def _(r=r):
            for i in range(10):
                zhalo[r, i] = tile

        for k, x_there in ((0, gx > 0), (1, gx < 7)):

            @pl.when(jnp.logical_and(z_there, jnp.logical_not(x_there)))
            def _(r=r, k=k):
                zhalo[r, 9 * k] = tile

        for e, y_there in ((0, gy > 0), (1, gy < 3)):
            both = jnp.logical_and(z_there, y_there)

            @pl.when(jnp.logical_not(both))
            def _(r=r, e=e):
                zcorner[r, e] = jnp.zeros((8, C), f32)

            for k, x_there in ((0, gx > 0), (1, gx < 7)):

                @pl.when(jnp.logical_not(jnp.logical_and(both, x_there)))
                def _(r=r, e=e, k=k):
                    zdot[r, e, k] = jnp.zeros((1, C), f32)

    pl.semaphore_wait(barrier, greeted + (4 + 12 + 31))

    def halo_copy(d):
        dx, dy, dz = d
        xs, xd = (None, None) if dx == 0 else ((0, 9) if dx < 0 else (LX - 1, 0))
        ys, yd = (None, None) if dy == 0 else ((0, 17) if dy < 0 else (LY - 1, 0))
        if dz == 0:
            if dy == 0:
                src, dst = cot_ref.at[xs], pad.at[1, xd, pl.ds(1, LY)]
            elif dx == 0:
                src, dst = cot_ref.at[:, ys], pad.at[1, pl.ds(1, LX), yd]
            else:
                src, dst = cot_ref.at[xs, ys], pad.at[1, xd, yd]
        else:
            s = 0 if dz < 0 else 1
            r = 1 - s
            if dy == 0:
                if dx == 0:
                    src, dst = zface.at[s], zhalo.at[r, pl.ds(1, LX)]
                else:
                    src, dst = zface.at[s, xs], zhalo.at[r, xd]
            else:
                e = 0 if dy < 0 else 1
                if dx == 0:
                    src, dst = zedge.at[s, e], zcorner.at[r, 1 - e]
                elif dx < 0:
                    src, dst = zpoint.at[s, e, 0], zdot.at[r, 1 - e, 1]
                else:
                    src, dst = zpoint.at[s, e, 1], zdot.at[r, 1 - e, 0]
        return remote(src, dst, hr.at[0 if dz == 0 else (2 if dz < 0 else 1)], dev(gx + dx, gy + dy, gz + dz))

    def send_part(device):
        here = part.at[gx * 4 + gy]
        remote(here, here, wr.at[1], device).start()

    to_plane(send_part)
    for d in DIRECTIONS:

        @pl.when(present(d))
        def _(d=d):
            halo_copy(d).start()

    near_x, near_y, near_z = count(gx, 7), count(gy, 3), count(gz, 7)

    def flat_rows(nx, ny):
        return 128 * nx + 64 * ny + 8 * nx * ny

    def wide_rows(nx, ny):
        return 64 + 8 * nx + 8 * ny + nx * ny

    def by_neighbours(rows, sem):
        for nx in (1, 2):
            for ny in (1, 2):

                @pl.when(jnp.logical_and(near_x == nx, near_y == ny))
                def _(nx=nx, ny=ny):
                    rows_wait(rows(nx, ny), sem)

    def wide_wait(late):
        for half in (0, 1):
            there = z_hi == half
            if not late:
                there = jnp.logical_and(there, near_z == 2)

            @pl.when(there)
            def _(half=half):
                by_neighbours(wide_rows, hr.at[1 + (1 - half if late else half)])

    for k in (2, 1, 3):
        remote(raw_ref, raws.at[gy], wr.at[0], gy_peer(k)).start()


    loads[2].wait()
    m = lax.broadcasted_iota(jnp.int32, (C, C), 0)
    col = lax.broadcasted_iota(jnp.int32, (C, C), 1)
    want = (m % 4) * 32 + (m // 4 + 16 * core) % 32
    order = jnp.where(col == want, 1.0, 0.0).astype(bf16)
    for j in range(4):
        xt[:, j * 512 : (j + 1) * 512] = lax.dot_general(
            order,
            x_ref[2 * j : 2 * j + 2].reshape(512, C),
            (((1,), (1,)), ((), ())),
            preferred_element_type=f32,
        ).astype(bf16)

    def widen(i, _):
        xf[pl.ds(pl.multiple_of(i * LY * LZ, LY * LZ), LY * LZ), :] = x_ref[i].reshape(LY * LZ, C).astype(f32)
        return 0

    lax.fori_loop(0, LX, widen, 0)
    xz[...] = lax.dot_general(
        order,
        xf[pl.ds(late_side * (LZ - 1), LX * LY, stride=LZ), :].astype(bf16),
        (((1,), (1,)), ((), ())),
        preferred_element_type=f32,
    ).astype(bf16)

    def tap_of(p):
        return p % 9 // 3, p % 3, (1, early_tap, late_tap)[p // 9]

    def pair_main(q, h):
        views = []
        for p in (4 * q + 2 * h, 4 * q + 2 * h + 1):
            if p < 27:
                a, b, c = tap_of(p)
                views.append(pad[c, 2 - a : 2 - a + LX, 2 - b : 2 - b + LY].reshape(CELLS, C))
        v = jnp.concatenate(views, axis=1) if len(views) == 2 else views[0]
        o = jnp.dot(xt[...], v, preferred_element_type=f32)
        return o if len(views) == 2 else jnp.concatenate([o, jnp.zeros((C, C), f32)], axis=1)

    def pair_rest(q, h):
        views = []
        for p in (4 * q + 2 * h, 4 * q + 2 * h + 1):
            if p < 27:
                a, b, _ = tap_of(p)
                views.append(turned[b, 2 - a : 2 - a + LX].reshape(LX * LY, C))
            else:
                views.append(jnp.zeros((LX * LY, C), bf16))
        return jnp.dot(xz[...], jnp.concatenate(views, axis=1), preferred_element_type=f32)

    def main(q):
        for h in range(2):
            base[2 * (q - 4) + h] = pair_main(q, h)

    def quad(q):
        outs = []
        for h in range(2):
            if q < 4:
                o = pair_main(q, h)
            else:
                o = base[2 * (q - 4) + h]
                if 4 * q + 2 * h >= 18:
                    o = o + pair_rest(q, h)
            outs += [o[:, :C], o[:, C:]]
        low = lax.broadcasted_iota(jnp.int32, (16, 8, C), 1) < 4
        pieces = [[], []]
        for h in range(2):
            one = outs[2 * h].reshape(16, 8, C)
            two = outs[2 * h + 1].reshape(16, 8, C)
            pieces[0].append(jnp.where(low, one, pltpu.roll(two, 4, 1)))
            pieces[1].append(jnp.where(low, pltpu.roll(one, 4, 1), two))
        for e in range(2):
            t = jnp.concatenate(pieces[e], axis=1)
            for j in range(8):
                own[q, 2 * j + e] = t[j]
                psend[q, 2 * j + e] = t[8 + j].astype(bf16)

    def quads(n):
        lo, hi = CHUNKS[n]
        for q in range(lo, hi):
            quad(q)
        some = pl.ds(lo, hi - lo)
        remote(psend.at[some], precv.at[some], dr.at[n], partner).start()

    def spread_chunk(n):
        lo, hi = CHUNKS[n]
        drain(precv.at[pl.ds(lo, hi - lo)], dr.at[n])
        for q in range(lo, hi):
            spread[:, q] = (own[q] + precv[q].astype(f32)).astype(bf16)

        for k in (10, 11, 9, 6, 14, 2, 8, 5, 7, 13, 15, 1, 3, 4, 12):
            remote(
                spread.at[at_gy[k // 4] * 4 + at_x[k % 4], pl.ds(lo, hi - lo)],
                r1.at[k - 1, pl.ds(lo, hi - lo)],
                got.at[1],
                xy_peer(k),
            ).start()

    by_neighbours(flat_rows, hr.at[0])
    quads(0)

    def lay_out(side):
        for i in range(10):
            plane[side, i, 8 : 8 + LY, :] = zhalo[side, i].astype(f32)
            for e, yr in ((0, 7), (1, 8 + LY)):
                if 0 < i < 9:
                    plane[side, i, yr : yr + 1, :] = zcorner[side, e, i - 1 : i, :]
                else:
                    plane[side, i, yr : yr + 1, :] = zdot[side, e, i // 9]

    def put_in(side):
        zr = 7 + 17 * side

        def put(i, _):
            full2[pl.ds(i * 18 * PITCH + zr, 18, stride=PITCH), :] = plane[side, i, 7 : 7 + 18, :]
            return 0

        lax.fori_loop(0, 10, put, 0)

    wide_wait(False)

    lay_out(early_side)
    put_in(early_side)
    for i in (0, 9):
        full[i, :, 8 : 8 + LZ, :] = pad[1, i].astype(f32)
    for j in (0, 17):
        full[1 : LX + 1, j, 8 : 8 + LZ, :] = pad[1, 1 : LX + 1, j].astype(f32)

    def shift(i, _):
        pad[0, i] = full[i, :, 9 : 9 + LZ, :].astype(bf16)
        pad[2, i] = full[i, :, 7 : 7 + LZ, :].astype(bf16)
        return 0

    lax.fori_loop(0, 10, shift, 0)
    quads(1)
    spread_chunk(0)
    for q in range(4, 7):
        main(q)
    drain(part.at[pl.ds(0, 31)], wr.at[1])
    drain(raws.at[pl.ds(0, 3)], wr.at[0])
    total = part[0]
    for j in range(1, 32):
        total = total + part[j]
    mean = total[0:1] / FAN
    var = total[1:2] / FAN - mean * mean
    inv = lax.rsqrt(var + var_eps)
    for t in range(27):
        for j in range(4):
            mine_raw[t, 4 * j : 4 * j + 4, :] = raws[j, t]
    mine_rows = pl.ds(pl.multiple_of(gx * 16, 16), 16)
    for p in range(27):
        a, b, c = TAPS[p]
        t = 9 * a + 3 * b + c
        w[mine_rows, p * C : (p + 1) * C] = ((mine_raw[t] - mean) * inv).astype(bf16)
    for t in range(27):
        mine_std[4 * t : 4 * t + 4, :] = (raw_ref[t] - mean) * inv

    halves = (slice(0, 14 * C), slice(14 * C, 27 * C))

    def slab(g, h):
        return w.at[pl.ds(pl.multiple_of(g * 16, 16), 16), halves[h]]

    for h in range(2):
        for step in (8, 1, 7):
            remote(slab(gx, h), slab(gx, h), wr.at[2 + h], chip_peer(step)).start()
    for h in range(2):
        remote(slab(gx, h), slab(gx, h), ours.at[h], partner).start()

    spread_chunk(1)
    wide_wait(True)
    lay_out(late_side)
    for i in range(10):
        turned[1, i] = zhalo[late_side, i]
        for b in (0, 2):
            turned[b, i] = plane[late_side, i, 9 - b : 9 - b + LY, :].astype(bf16)
    quads(2)
    spread_chunk(2)
    def hand_on(h):
        drain(w.at[pl.ds(0, 48), halves[h]], wr.at[2 + h])
        for k in (1, 2, 3):
            g = at_gx[k][0]
            remote(slab(g, h), slab(g, h), ours.at[h], partner).start()

    def take_over(h):
        drain(w.at[pl.ds(0, 64), halves[h]], ours.at[h])
        for p in range(14 * h, 14 + 13 * h):
            wt[p * C : (p + 1) * C, :] = w[:, p * C : (p + 1) * C].T

    def input_grad(h, lo, hi):
        def one(i, _):
            views = []
            for a, b, c in TAPS[14 * h : 14 + 13 * h]:
                views.append(pad[c, i + 2 - a, 2 - b : 2 - b + LY].reshape(LY * LZ, C))
            out = jnp.dot(jnp.concatenate(views, axis=1), wt[halves[h], :], preferred_element_type=f32)
            if h == 0:
                part_dx[i] = out
            else:
                dx_ref[i] = (part_dx[i] + out).astype(bf16).reshape(LY, LZ, C)
            return 0

        lax.fori_loop(lo, hi, one, 0)

    put_in(late_side)
    lax.fori_loop(0, 10, shift, 0)
    drain(r1, got.at[1])
    for q in range(7):
        acc = own[q, mine] + precv[q, mine].astype(f32)
        for k in range(15):
            acc = acc + r1[k, q].astype(f32)
        red[q * 16 : (q + 1) * 16, :] = acc
    for j in range(4):
        for n, start in enumerate((0, 72 - 36 * z_hi, 36 + 36 * z_hi)):
            comp[j, 9 * n : 9 * n + 9, :] = red[pl.ds(start + j, 9, stride=4), :]
        comp[j, 27:32, :] = jnp.zeros((5, C), f32)
        rows[j] = comp[j].astype(bf16)
    r2[z] = rows[z_lo]

    for k in (4, 3, 5, 2, 6, 1, 7):
        remote(rows.at[spots[k][0]], r2.at[z], got.at[2], z_peer(k)).start()

    hand_on(0)
    take_over(0)
    input_grad(0, 0, 8)
    hand_on(1)
    drain(r2.at[pl.ds(0, 7)], got.at[2])
    acc = r2[0].astype(f32)
    for j in range(1, 8):
        acc = acc + r2[j].astype(f32)
    gath[x] = acc

    for k in (2, 1, 3):
        remote(gath.at[x], gath.at[x], got.at[3], x_peer(k)).start()
    take_over(1)
    input_grad(1, 0, 4)

    drain(gath.at[pl.ds(0, 3)], got.at[3])
    for r in range(4):
        for n, c in enumerate((1, 0, 2)):
            nat[pl.ds(4 * c + r, 9, stride=12), :] = gath[r, n * 9 : n * 9 + 9, :]
    g = nat[0:108, :]
    std = mine_std[0:108, :]
    here = gx * 4 + gy
    stat[here, 0:1, :] = jnp.sum(g, axis=0, keepdims=True)
    stat[here, 1:2, :] = jnp.sum(g * std, axis=0, keepdims=True)
    stat[here, 2:3, :] = jnp.sum(g * g, axis=0, keepdims=True)
    stat[here, 3:4, :] = jnp.zeros((1, C), f32)

    def send_stat(device):
        remote(stat.at[here], stat.at[here], got.at[4], device).start()

    to_plane(send_stat)
    input_grad(1, 4, 8)
    drain(stat.at[pl.ds(0, 31)], got.at[4])
    total = stat[0]
    for j in range(1, 32):
        total = total + stat[j]
    sum_grad, sum_cross, sum_square = total[0:1], total[1:2], total[2:3]
    mean_grad = sum_grad / FAN
    mean_cross = sum_cross / FAN
    per_output = sum_square - 2.0 * mean_grad * sum_grad - 2.0 * mean_cross * sum_cross
    per_output = (
        per_output + FAN * mean_grad * mean_grad + FAN * mean_cross * mean_cross * var / (var + var_eps)
    )
    square_sum = jnp.sum(inv * inv * per_output, axis=1, keepdims=True)
    scale = jnp.minimum(1.0, clip_norm * lax.rsqrt(square_sum + norm_eps))
    factor = inv * scale
    for t in range(27):
        g = nat[4 * t : 4 * t + 4, :]
        dw_ref[t] = factor * (g - mean_grad - mine_std[4 * t : 4 * t + 4, :] * mean_cross)

    always = (3 * 27 * 4 * C + 31 * 2 * C + 31 * 4 * C + 3 * 32 * C) * 4 + (
        7 * 16 * 27 * C + 7 * 256 * C + 15 * 112 * C + 7 * 32 * C
    ) * 2
    for nz in (1, 2):

        @pl.when(near_z == nz)
        def _(nz=nz):
            by_neighbours(
                lambda nx, ny: flat_rows(nx, ny) + nz * wide_rows(nx, ny) + always // (4 * C), sent.at[0]
            )


def hand_over(dx_in, dw_in, dx_out, dw_out, sems):
    copies = [
        pltpu.make_async_copy(a, b, sems.at[n]) for n, (a, b) in enumerate(((dx_in, dx_out), (dw_in, dw_out)))
    ]
    for copy in copies:
        copy.start()
    for copy in copies:
        copy.wait()


def on_device(raw_weight, inputs, cotangent):
    dma = pltpu.SemaphoreType.DMA
    vmem = pltpu.VMEM
    dx, dw = pl.pallas_call(
        body,
        out_shape=(
            pltpu.VMEM(inputs.shape, bf16),
            pltpu.VMEM((27, 4, C), f32),
        ),
        in_specs=[pl.BlockSpec(memory_space=pltpu.HBM)] * 3,
        out_specs=[pl.BlockSpec(memory_space=pltpu.VMEM)] * 2,
        scratch_shapes=[
            vmem((27, 4, C), f32),
            vmem((LX, LY, LZ, C), bf16),
            vmem((LX, LY, LZ, C), bf16),
            vmem((10, 18, PITCH, C), f32),
            vmem((3, 10, 18, LZ, C), bf16),
            vmem((2, LX, LY, C), bf16),
            vmem((2, 2, 8, C), f32),
            vmem((2, 2, 2, 1, C), f32),
            vmem((2, 10, LY, C), bf16),
            vmem((2, 2, 8, C), f32),
            vmem((2, 2, 2, 1, C), f32),
            vmem((2, 10, 32, C), f32),
            vmem((3, 10, LY, C), bf16),
            vmem((CELLS, C), f32),
            vmem((C, CELLS), bf16),
            vmem((C, C), bf16),
            vmem((6, C, 2 * C), f32),
            vmem((4, 27, 4, C), f32),
            vmem((27, 16, C), f32),
            vmem((32, 2, C), f32),
            vmem((C, 27 * C), bf16),
            vmem((27 * C, C), bf16),
            vmem((LX, LY * LZ, C), f32),
            vmem((7, 16, 16, C), f32),
            vmem((7, 16, 16, C), bf16),
            vmem((7, 16, 16, C), bf16),
            vmem((16, 7, 16, C), bf16),
            vmem((15, 7, 16, C), bf16),
            vmem((112, C), f32),
            vmem((4, 32, C), f32),
            vmem((8, 32, C), bf16),
            vmem((4, 32, C), bf16),
            vmem((4, 32, C), f32),
            vmem((112, C), f32),
            vmem((112, C), f32),
            vmem((32, 4, C), f32),
            dma((3,)),
            dma((3,)),
            dma((4,)),
            dma((3,)),
            dma((2,)),
            dma((5,)),
            dma((1,)),
        ],
        compiler_params=pltpu.CompilerParams(
            collective_id=0, has_side_effects=True, vmem_limit_bytes=40 * 1024 * 1024
        ),
    )(*[pltpu.with_memory_space_constraint(a, pltpu.HBM) for a in (jnp.swapaxes(raw_weight, 0, 1), inputs, cotangent)])
    dx, dw = pl.pallas_call(
        hand_over,
        out_shape=(jax.ShapeDtypeStruct(dx.shape, bf16), jax.ShapeDtypeStruct(dw.shape, f32)),
        in_specs=[pl.BlockSpec(memory_space=pltpu.VMEM)] * 2,
        out_specs=[pl.BlockSpec(memory_space=pl.ANY)] * 2,
        scratch_shapes=[dma((2,))],
    )(*[pltpu.with_memory_space_constraint(a, pltpu.VMEM) for a in (dx, dw)])
    return dx, jnp.swapaxes(dw, 0, 1)


def solution(mesh):
    in_specs = (P(("gx", "gy"), None, None), P("gx", "gy", "gz", None), P("gx", "gy", "gz", None))
    out_specs = (P("gx", "gy", "gz", None), P(("gx", "gy"), None, None))
    return jax.shard_map(
        on_device, mesh=mesh, in_specs=in_specs, out_specs=out_specs, check_vma=False
    )
```

```python
import functools

import jax
import jax.numpy as jnp
from jax import lax
from jax.experimental import pallas as pl
from jax.experimental.pallas import tpu as pltpu
from jax.sharding import PartitionSpec as P

var_eps = 1e-05
norm_eps = 1e-06
clip_norm = 600.0

f32 = jnp.float32
bf16 = jnp.bfloat16
MESH = pl.DeviceIdType.MESH

C = 128
LX, LY, LZ = 8, 16, 16
CELLS = LX * LY * LZ
PITCH = 32
FAN = 27 * C

TAPS = [(t // 9, t // 3 % 3, t % 3) for t in range(27)]
CHUNKS = ((0, 2), (2, 4), (4, 7))
DIRECTIONS = [
    (dx, dy, dz)
    for dz in (-1, 1, 0)
    for dx in (0, -1, 1)
    for dy in (0, -1, 1)
    if (dx, dy, dz) != (0, 0, 0)
]


def body(raw_hbm, x_hbm, cot_hbm, dx_ref, dw_ref, raw_ref, x_ref, cot_ref,
         full, pad, zface, zedge, zpoint, zhalo, zcorner, zdot, plane, turned, xf, xt, xy, xz, grad, land_x, land_y, land_c,
         raws, mine_raw, part, w, wt, part_dx, own, psend, precv, spread, r1, red, comp, r2, rows, gath, nat, mine_std, stat,
         ls, hr, wr, dr, ours, got, sent):
    gx, gy, gz = lax.axis_index("gx"), lax.axis_index("gy"), lax.axis_index("gz")
    def div(a, n):
        return lax.div(a, jnp.int32(n))

    def mod(a, n):
        return lax.rem(a, jnp.int32(n))

    z_lo, core = div(gx, 2), mod(gx, 2)
    z_hi, x = div(gz, 4), mod(gz, 4)
    z = z_hi * 4 + z_lo
    mine = gy * 4 + x
    early_tap, late_tap = 2 - 2 * z_hi, 2 * z_hi
    early_side, late_side = z_hi, 1 - z_hi
    full2 = full.reshape(10 * 18 * PITCH, C)

    def dev(a, b, c):
        return (a, b, c)

    def ring(step):
        zz = mod(z + step, 8)
        return mod(zz, 4), div(zz, 4)

    spots = [ring(step) for step in range(8)] + [ring(2 + 4 * core)]
    at_gz = [hi * 4 + x for _, hi in spots]
    at_gx = [[lo * 2 + core, lo * 2 + 1 - core] for lo, _ in spots]
    at_gy = [gy] + [mod(gy + k, 4) for k in range(1, 4)]
    at_x = [x] + [mod(x + k, 4) for k in range(1, 4)]
    x_gz = [gz] + [z_hi * 4 + at_x[k] for k in range(1, 4)]

    def chip_peer(step):
        return dev(at_gx[step][0], gy, at_gz[step])

    def gy_peer(k):
        return dev(gx, at_gy[k], gz)

    def x_peer(k):
        return dev(gx, gy, x_gz[k])

    def xy_peer(k):
        return dev(gx, at_gy[k // 4], x_gz[k % 4])

    z_peer = chip_peer
    def plane_peer(k, step):
        return dev(at_gx[step][k // 4], at_gy[k % 4], at_gz[step])

    def to_plane(send, steps=(2, 1, 7, 0)):
        for step in steps:
            for k in range(1 if step == 0 else 0, 8):
                send(plane_peer(k, step))

    partner = dev(gx + 1 - 2 * core, gy, gz)

    def remote(src, dst, recv, device):
        return pltpu.make_async_remote_copy(
            src_ref=src, dst_ref=dst, send_sem=sent.at[0], recv_sem=recv, device_id=device, device_id_type=MESH
        )

    def rows_wait(n, sem):
        view = full2.at[pl.ds(0, n)]
        pltpu.make_async_copy(view, view, sem).wait()

    def drain(ref, sem):
        pltpu.make_async_copy(ref, ref, sem).wait()

    def exists(axis_index, last, step):
        if step == 0:
            return None
        return axis_index > 0 if step < 0 else axis_index < last

    def count(axis_index, last):
        return (axis_index > 0).astype(jnp.int32) + (axis_index < last).astype(jnp.int32)

    def present(d):
        tests = [exists(gx, 7, d[0]), exists(gy, 3, d[1]), exists(gz, 7, d[2])]
        tests = [t for t in tests if t is not None]
        out = tests[0]
        for t in tests[1:]:
            out = jnp.logical_and(out, t)
        return out

    loads = [
        pltpu.make_async_copy(a, b, ls.at[n])
        for n, (a, b) in enumerate(((cot_hbm, cot_ref), (raw_hbm, raw_ref), (x_hbm, x_ref)))
    ]
    for load in loads:
        load.start()

    barrier = pltpu.get_barrier_semaphore()

    def greet(device):
        pl.semaphore_signal(barrier, inc=1, device_id=device, device_id_type=MESH)

    wide = [d for d in DIRECTIONS if d[2] != 0]
    greeted = jnp.int32(0)
    for d in wide:
        there = present(d)

        @pl.when(there)
        def _(d=d):
            greet(dev(gx + d[0], gy + d[1], gz + d[2]))

        greeted = greeted + there.astype(jnp.int32)
    for k in (4, 3, 5, 2):
        greet(z_peer(k))
    for k in (10, 11, 9, 6, 14, 5, 7, 13, 15, 1, 2, 3):
        greet(xy_peer(k))
    to_plane(greet, (6, 1, 7, 0))

    loads[0].wait()

    def fill(i, _):
        slab = cot_ref[i]
        pad[1, i + 1, 1 : LY + 1] = slab
        full[i + 1, 1 : LY + 1, 8 : 8 + LZ, :] = slab.astype(f32)
        return 0

    lax.fori_loop(0, LX, fill, 0)

    def faces(i, _):
        for s, zr in ((0, 8), (1, 8 + LZ - 1)):
            zface[s, i] = full2[pl.ds(((i + 1) * 18 + 1) * PITCH + zr, LY, stride=PITCH), :].astype(bf16)
        return 0

    lax.fori_loop(0, LX, faces, 0)
    for s, zr in ((0, 8), (1, 8 + LZ - 1)):
        for e, yr in ((0, 1), (1, LY)):
            for i in range(LX):
                at = ((i + 1) * 18 + yr) * PITCH + zr
                zedge[s, e, i : i + 1, :] = full2[at : at + 1, :]
            zpoint[s, e, 0] = zedge[s, e, 0:1, :]
            zpoint[s, e, 1] = zedge[s, e, LX - 1 : LX, :]
    loads[1].wait()
    raws[gy] = raw_ref[...]
    first = jnp.zeros((4, C), f32)
    second = jnp.zeros((4, C), f32)
    for t in range(27):
        v = raw_ref[t]
        first = first + v
        second = second + v * v
    part[gx * 4 + gy, 0:1, :] = jnp.sum(first, axis=0, keepdims=True)
    part[gx * 4 + gy, 1:2, :] = jnp.sum(second, axis=0, keepdims=True)

    pl.semaphore_wait(barrier, greeted + (4 + 12 + 31))

    def halo_copy(d):
        dx, dy, dz = d
        xs, xd = (None, None) if dx == 0 else ((0, 1) if dx < 0 else (LX - 1, 0))
        ys, yd = (None, None) if dy == 0 else ((0, 1) if dy < 0 else (LY - 1, 0))
        if dz == 0:
            if dy == 0:
                src, dst = cot_ref.at[xs], land_x.at[xd]
            elif dx == 0:
                src, dst = cot_ref.at[:, ys], land_y.at[yd]
            else:
                src, dst = cot_ref.at[xs, ys], land_c.at[xd, yd]
        else:
            s = 0 if dz < 0 else 1
            r = 1 - s
            if dy == 0:
                if dx == 0:
                    src, dst = zface.at[s], zhalo.at[r, pl.ds(1, LX)]
                else:
                    src, dst = zface.at[s, xs], zhalo.at[r, 9 * xd]
            else:
                e = 0 if dy < 0 else 1
                if dx == 0:
                    src, dst = zedge.at[s, e], zcorner.at[r, 1 - e]
                elif dx < 0:
                    src, dst = zpoint.at[s, e, 0], zdot.at[r, 1 - e, 1]
                else:
                    src, dst = zpoint.at[s, e, 1], zdot.at[r, 1 - e, 0]
        return remote(src, dst, hr.at[0 if dz == 0 else (2 if dz < 0 else 1)], dev(gx + dx, gy + dy, gz + dz))

    def send_part(device):
        here = part.at[gx * 4 + gy]
        remote(here, here, wr.at[1], device).start()

    for d in DIRECTIONS:

        @pl.when(present(d))
        def _(d=d):
            halo_copy(d).start()

    near_x, near_y, near_z = count(gx, 7), count(gy, 3), count(gz, 7)

    def flat_rows(nx, ny):
        return 128 * nx + 64 * ny + 8 * nx * ny

    def wide_rows(nx, ny):
        return 64 + 8 * nx + 8 * ny + nx * ny

    def by_neighbours(rows, sem):
        for nx in (1, 2):
            for ny in (1, 2):

                @pl.when(jnp.logical_and(near_x == nx, near_y == ny))
                def _(nx=nx, ny=ny):
                    rows_wait(rows(nx, ny), sem)

    def wide_wait(late):
        for half in (0, 1):
            there = z_hi == half
            if not late:
                there = jnp.logical_and(there, near_z == 2)

            @pl.when(there)
            def _(half=half):
                by_neighbours(wide_rows, hr.at[1 + (1 - half if late else half)])

    for k in (2, 1, 3):
        remote(raw_ref, raws.at[gy], wr.at[0], gy_peer(k)).start()
    to_plane(send_part)

    tile = jnp.zeros((LZ, C), bf16)

    for c in range(3):
        for i in (0, 9):
            for j in range(18):
                pad[c, i, j] = tile
        for i in range(1, 9):
            pad[c, i, 0] = tile
            pad[c, i, 17] = tile

    for k, x_there in ((0, gx > 0), (1, gx < 7)):

        @pl.when(jnp.logical_not(x_there))
        def _(k=k):
            for j in range(LY):
                land_x[k, j] = tile

        for e, y_there in ((0, gy > 0), (1, gy < 3)):

            @pl.when(jnp.logical_not(jnp.logical_and(x_there, y_there)))
            def _(k=k, e=e):
                land_c[k, e] = tile

    for e, y_there in ((0, gy > 0), (1, gy < 3)):

        @pl.when(jnp.logical_not(y_there))
        def _(e=e):
            for i in range(LX):
                land_y[e, i] = tile

    for r, z_there in ((0, gz > 0), (1, gz < 7)):

        @pl.when(jnp.logical_not(z_there))
        def _(r=r):
            for i in range(10):
                zhalo[r, i] = tile

        for k, x_there in ((0, gx > 0), (1, gx < 7)):

            @pl.when(jnp.logical_and(z_there, jnp.logical_not(x_there)))
            def _(r=r, k=k):
                zhalo[r, 9 * k] = tile

        for e, y_there in ((0, gy > 0), (1, gy < 3)):
            both = jnp.logical_and(z_there, y_there)

            @pl.when(jnp.logical_not(both))
            def _(r=r, e=e):
                zcorner[r, e] = jnp.zeros((8, C), f32)

            for k, x_there in ((0, gx > 0), (1, gx < 7)):

                @pl.when(jnp.logical_not(jnp.logical_and(both, x_there)))
                def _(r=r, e=e, k=k):
                    zdot[r, e, k] = jnp.zeros((1, C), f32)

    for i in range(10):
        for zr in (7, 8 + LZ):
            full2[pl.ds(i * 18 * PITCH + zr, 18, stride=PITCH), :] = jnp.zeros((18, C), f32)

    def shift(i, _):
        pad[0, i] = full[i, :, 9 : 9 + LZ, :].astype(bf16)
        pad[2, i] = full[i, :, 7 : 7 + LZ, :].astype(bf16)
        return 0

    def shift_inside(i, _):
        inside = slice(1, LY + 1)
        pad[0, i, inside] = full[i, inside, 9 : 9 + LZ, :].astype(bf16)
        pad[2, i, inside] = full[i, inside, 7 : 7 + LZ, :].astype(bf16)
        return 0

    lax.fori_loop(1, LX + 1, shift_inside, 0)
    loads[2].wait()
    m = lax.broadcasted_iota(jnp.int32, (C, C), 0)
    col = lax.broadcasted_iota(jnp.int32, (C, C), 1)
    want = (m % 4) * 32 + (m // 4 + 16 * core) % 32
    order = jnp.where(col == want, 1.0, 0.0).astype(bf16)
    for j in range(4):
        xt[:, j * 512 : (j + 1) * 512] = lax.dot_general(
            order,
            x_ref[2 * j : 2 * j + 2].reshape(512, C),
            (((1,), (1,)), ((), ())),
            preferred_element_type=f32,
        ).astype(bf16)

    def widen(i, _):
        xf[pl.ds(pl.multiple_of(i * LY * LZ, LY * LZ), LY * LZ), :] = x_ref[i].reshape(LY * LZ, C).astype(f32)
        return 0

    lax.fori_loop(0, LX, widen, 0)
    def by_channel(cells):
        return lax.dot_general(order, cells, (((1,), (1,)), ((), ())), preferred_element_type=f32).astype(bf16)

    for n, e in ((0, 0), (1, LZ - 1)):
        xy[n] = by_channel(x_ref[:, e].reshape(LX * LZ, C))
        xz[n] = by_channel(xf[pl.ds(e, LX * LY, stride=LZ), :].astype(bf16))

    def tap_of(p):
        return p % 9 // 3, p % 3, (1, early_tap, late_tap)[p // 9]

    for p in range(0, 27, 2):
        views = []
        for t in range(p, min(p + 2, 27)):
            a, b, c = tap_of(t)
            views.append(pad[c, 2 - a : 2 - a + LX, 2 - b : 2 - b + LY].reshape(CELLS, C))
        v = jnp.concatenate(views, axis=1) if len(views) == 2 else views[0]
        o = jnp.dot(xt[...], v, preferred_element_type=f32)
        for n in range(len(views)):
            grad[p + n] = o[:, n * C : (n + 1) * C]
    grad[27] = jnp.zeros((C, C), f32)

    def add_side(lhs, taps, view):
        o = jnp.dot(lhs, jnp.concatenate([view(p) for p in taps], axis=1), preferred_element_type=f32)
        for n, p in enumerate(taps):
            grad[p] += o[:, n * C : (n + 1) * C]

    def quad(q):
        outs = [grad[p] for p in range(4 * q, 4 * q + 4)]
        low = lax.broadcasted_iota(jnp.int32, (16, 8, C), 1) < 4
        pieces = [[], []]
        for h in range(2):
            one = outs[2 * h].reshape(16, 8, C)
            two = outs[2 * h + 1].reshape(16, 8, C)
            pieces[0].append(jnp.where(low, one, pltpu.roll(two, 4, 1)))
            pieces[1].append(jnp.where(low, pltpu.roll(one, 4, 1), two))
        for e in range(2):
            t = jnp.concatenate(pieces[e], axis=1)
            for j in range(8):
                own[q, 2 * j + e] = t[j]
                psend[q, 2 * j + e] = t[8 + j].astype(bf16)

    def quads(n):
        lo, hi = CHUNKS[n]
        for q in range(lo, hi):
            quad(q)
        some = pl.ds(lo, hi - lo)
        remote(psend.at[some], precv.at[some], dr.at[n], partner).start()

    def spread_chunk(n):
        lo, hi = CHUNKS[n]
        drain(precv.at[pl.ds(lo, hi - lo)], dr.at[n])
        for q in range(lo, hi):
            spread[:, q] = (own[q] + precv[q].astype(f32)).astype(bf16)

        for k in (10, 11, 9, 6, 14, 2, 8, 5, 7, 13, 15, 1, 3, 4, 12):
            remote(
                spread.at[at_gy[k // 4] * 4 + at_x[k % 4], pl.ds(lo, hi - lo)],
                r1.at[k - 1, pl.ds(lo, hi - lo)],
                got.at[1],
                xy_peer(k),
            ).start()

    by_neighbours(flat_rows, hr.at[0])
    for e, yr in ((0, 0), (1, LY + 1)):
        face = land_y[e]
        pad[1, 1 : LX + 1, yr] = face
        full[1 : LX + 1, yr, 8 : 8 + LZ, :] = face.astype(f32)
        pad[0, 1 : LX + 1, yr] = full[1 : LX + 1, yr, 9 : 9 + LZ, :].astype(bf16)
        pad[2, 1 : LX + 1, yr] = full[1 : LX + 1, yr, 7 : 7 + LZ, :].astype(bf16)

        def view_y(p, yr=yr):
            a, _, c = tap_of(p)
            return pad[c, 2 - a : 2 - a + LX, yr].reshape(LX * LZ, C)

        add_side(xy[e], [p for p in range(27) if p % 3 == (2 if e == 0 else 0)], view_y)
    for k, xr in ((0, 0), (1, LX + 1)):
        pad[1, xr, 1 : LY + 1] = land_x[k]
        full[xr, 1 : LY + 1, 8 : 8 + LZ, :] = land_x[k].astype(f32)
        for e, yr in ((0, 0), (1, LY + 1)):
            pad[1, xr, yr] = land_c[k, e]
            full[xr, yr, 8 : 8 + LZ, :] = land_c[k, e].astype(f32)
        shift(xr, 0)

        def view_x(p, xr=xr):
            _, b, c = tap_of(p)
            return pad[c, xr, 2 - b : 2 - b + LY].reshape(LY * LZ, C)

        cells = LY * LZ
        lhs = xt[:, :cells] if k == 0 else xt[:, CELLS - cells :]
        add_side(lhs, [p for p in range(27) if p % 9 // 3 == (2 if k == 0 else 0)], view_x)
    quads(0)
    def lay_out(side):
        for i in range(10):
            plane[side, i, 8 : 8 + LY, :] = zhalo[side, i].astype(f32)
            for e, yr in ((0, 7), (1, 8 + LY)):
                if 0 < i < 9:
                    plane[side, i, yr : yr + 1, :] = zcorner[side, e, i - 1 : i, :]
                else:
                    plane[side, i, yr : yr + 1, :] = zdot[side, e, i // 9]
        for i in range(10):
            turned[1, i] = zhalo[side, i]
            for b in (0, 2):
                turned[b, i] = plane[side, i, 9 - b : 9 - b + LY, :].astype(bf16)

    def put_in(side):
        zr = 7 + 17 * side

        def put(i, _):
            full2[pl.ds(i * 18 * PITCH + zr, 18, stride=PITCH), :] = plane[side, i, 7 : 7 + 18, :]
            return 0

        lax.fori_loop(0, 10, put, 0)

    def view_z(p):
        a, b, _ = tap_of(p)
        return turned[b, 2 - a : 2 - a + LX].reshape(LX * LY, C)

    wide_wait(False)
    lay_out(early_side)
    add_side(xz[early_side], range(9, 18), view_z)
    quads(1)
    spread_chunk(0)
    drain(part.at[pl.ds(0, 31)], wr.at[1])
    drain(raws.at[pl.ds(0, 3)], wr.at[0])
    total = part[0]
    for j in range(1, 32):
        total = total + part[j]
    mean = total[0:1] / FAN
    var = total[1:2] / FAN - mean * mean
    inv = lax.rsqrt(var + var_eps)
    for t in range(27):
        for j in range(4):
            mine_raw[t, 4 * j : 4 * j + 4, :] = raws[j, t]
    mine_rows = pl.ds(pl.multiple_of(gx * 16, 16), 16)
    for p in range(27):
        a, b, c = TAPS[p]
        t = 9 * a + 3 * b + c
        w[mine_rows, p * C : (p + 1) * C] = ((mine_raw[t] - mean) * inv).astype(bf16)
    for t in range(27):
        mine_std[4 * t : 4 * t + 4, :] = (raw_ref[t] - mean) * inv

    halves = (slice(0, 14 * C), slice(14 * C, 27 * C))

    def slab(g, h):
        return w.at[pl.ds(pl.multiple_of(g * 16, 16), 16), halves[h]]

    for h in range(2):
        for step in (8, 1, 7):
            remote(slab(gx, h), slab(gx, h), wr.at[2 + h], chip_peer(step)).start()
    for h in range(2):
        remote(slab(gx, h), slab(gx, h), ours.at[h], partner).start()

    spread_chunk(1)
    wide_wait(True)
    lay_out(late_side)
    add_side(xz[late_side], range(18, 27), view_z)
    quads(2)
    spread_chunk(2)
    def hand_on(h):
        drain(w.at[pl.ds(0, 48), halves[h]], wr.at[2 + h])
        for k in (1, 2, 3):
            g = at_gx[k][0]
            remote(slab(g, h), slab(g, h), ours.at[h], partner).start()

    def take_over(h):
        drain(w.at[pl.ds(0, 64), halves[h]], ours.at[h])
        for p in range(14 * h, 14 + 13 * h):
            wt[p * C : (p + 1) * C, :] = w[:, p * C : (p + 1) * C].T

    def input_grad(h, lo, hi):
        def one(i, _):
            views = []
            for a, b, c in TAPS[14 * h : 14 + 13 * h]:
                views.append(pad[c, pl.ds(2 * i + 2 - a, 2), 2 - b : 2 - b + LY].reshape(2 * LY * LZ, C))
            out = jnp.dot(jnp.concatenate(views, axis=1), wt[halves[h], :], preferred_element_type=f32)
            if h == 0:
                part_dx[i] = out
            else:
                dx_ref[pl.ds(2 * i, 2)] = (part_dx[i] + out).astype(bf16).reshape(2, LY, LZ, C)
            return 0

        lax.fori_loop(lo, hi, one, 0)

    put_in(0)
    put_in(1)
    lax.fori_loop(0, 10, shift, 0)
    hand_on(0)
    drain(r1, got.at[1])
    for q in range(7):
        acc = own[q, mine] + precv[q, mine].astype(f32)
        for k in range(15):
            acc = acc + r1[k, q].astype(f32)
        red[q * 16 : (q + 1) * 16, :] = acc
    for j in range(4):
        for n, start in enumerate((0, 72 - 36 * z_hi, 36 + 36 * z_hi)):
            comp[j, 9 * n : 9 * n + 9, :] = red[pl.ds(start + j, 9, stride=4), :]
        comp[j, 27:32, :] = jnp.zeros((5, C), f32)
        rows[j] = comp[j].astype(bf16)
    r2[z] = rows[z_lo]

    for k in (4, 3, 5, 2, 6, 1, 7):
        remote(rows.at[spots[k][0]], r2.at[z], got.at[2], z_peer(k)).start()

    take_over(0)
    input_grad(0, 0, 4)
    hand_on(1)
    drain(r2.at[pl.ds(0, 7)], got.at[2])
    acc = r2[0].astype(f32)
    for j in range(1, 8):
        acc = acc + r2[j].astype(f32)
    gath[x] = acc

    for k in (2, 1, 3):
        remote(gath.at[x], gath.at[x], got.at[3], x_peer(k)).start()
    take_over(1)
    input_grad(1, 0, 2)

    drain(gath.at[pl.ds(0, 3)], got.at[3])
    for r in range(4):
        for n, c in enumerate((1, 0, 2)):
            nat[pl.ds(4 * c + r, 9, stride=12), :] = gath[r, n * 9 : n * 9 + 9, :]
    g = nat[0:108, :]
    std = mine_std[0:108, :]
    here = gx * 4 + gy
    stat[here, 0:1, :] = jnp.sum(g, axis=0, keepdims=True)
    stat[here, 1:2, :] = jnp.sum(g * std, axis=0, keepdims=True)
    stat[here, 2:3, :] = jnp.sum(g * g, axis=0, keepdims=True)
    stat[here, 3:4, :] = jnp.zeros((1, C), f32)

    def send_stat(device):
        remote(stat.at[here], stat.at[here], got.at[4], device).start()

    to_plane(send_stat)
    input_grad(1, 2, 4)
    drain(stat.at[pl.ds(0, 31)], got.at[4])
    total = stat[0]
    for j in range(1, 32):
        total = total + stat[j]
    sum_grad, sum_cross, sum_square = total[0:1], total[1:2], total[2:3]
    mean_grad = sum_grad / FAN
    mean_cross = sum_cross / FAN
    per_output = sum_square - 2.0 * mean_grad * sum_grad - 2.0 * mean_cross * sum_cross
    per_output = (
        per_output + FAN * mean_grad * mean_grad + FAN * mean_cross * mean_cross * var / (var + var_eps)
    )
    square_sum = jnp.sum(inv * inv * per_output, axis=1, keepdims=True)
    scale = jnp.minimum(1.0, clip_norm * lax.rsqrt(square_sum + norm_eps))
    factor = inv * scale
    for t in range(27):
        g = nat[4 * t : 4 * t + 4, :]
        dw_ref[t] = factor * (g - mean_grad - mine_std[4 * t : 4 * t + 4, :] * mean_cross)

    always = (3 * 27 * 4 * C + 31 * 2 * C + 31 * 4 * C + 3 * 32 * C) * 4 + (
        7 * 16 * 27 * C + 7 * 256 * C + 15 * 112 * C + 7 * 32 * C
    ) * 2
    for nz in (1, 2):

        @pl.when(near_z == nz)
        def _(nz=nz):
            by_neighbours(
                lambda nx, ny: flat_rows(nx, ny) + nz * wide_rows(nx, ny) + always // (4 * C), sent.at[0]
            )


def hand_over(dx_in, dw_in, dx_out, dw_out, sems):
    copies = [
        pltpu.make_async_copy(a, b, sems.at[n]) for n, (a, b) in enumerate(((dx_in, dx_out), (dw_in, dw_out)))
    ]
    for copy in copies:
        copy.start()
    for copy in copies:
        copy.wait()


def on_device(raw_weight, inputs, cotangent):
    dma = pltpu.SemaphoreType.DMA
    vmem = pltpu.VMEM
    dx, dw = pl.pallas_call(
        body,
        out_shape=(
            pltpu.VMEM(inputs.shape, bf16),
            pltpu.VMEM((27, 4, C), f32),
        ),
        in_specs=[pl.BlockSpec(memory_space=pltpu.HBM)] * 3,
        out_specs=[pl.BlockSpec(memory_space=pltpu.VMEM)] * 2,
        scratch_shapes=[
            vmem((27, 4, C), f32),
            vmem((LX, LY, LZ, C), bf16),
            vmem((LX, LY, LZ, C), bf16),
            vmem((10, 18, PITCH, C), f32),
            vmem((3, 10, 18, LZ, C), bf16),
            vmem((2, LX, LY, C), bf16),
            vmem((2, 2, 8, C), f32),
            vmem((2, 2, 2, 1, C), f32),
            vmem((2, 10, LY, C), bf16),
            vmem((2, 2, 8, C), f32),
            vmem((2, 2, 2, 1, C), f32),
            vmem((2, 10, 32, C), f32),
            vmem((3, 10, LY, C), bf16),
            vmem((CELLS, C), f32),
            vmem((C, CELLS), bf16),
            vmem((2, C, C), bf16),
            vmem((2, C, C), bf16),
            vmem((28, C, C), f32),
            vmem((2, LY, LZ, C), bf16),
            vmem((2, LX, LZ, C), bf16),
            vmem((2, 2, LZ, C), bf16),
            vmem((4, 27, 4, C), f32),
            vmem((27, 16, C), f32),
            vmem((32, 2, C), f32),
            vmem((C, 27 * C), bf16),
            vmem((27 * C, C), bf16),
            vmem((LX // 2, 2 * LY * LZ, C), f32),
            vmem((7, 16, 16, C), f32),
            vmem((7, 16, 16, C), bf16),
            vmem((7, 16, 16, C), bf16),
            vmem((16, 7, 16, C), bf16),
            vmem((15, 7, 16, C), bf16),
            vmem((112, C), f32),
            vmem((4, 32, C), f32),
            vmem((8, 32, C), bf16),
            vmem((4, 32, C), bf16),
            vmem((4, 32, C), f32),
            vmem((112, C), f32),
            vmem((112, C), f32),
            vmem((32, 4, C), f32),
            dma((3,)),
            dma((3,)),
            dma((4,)),
            dma((3,)),
            dma((2,)),
            dma((5,)),
            dma((1,)),
        ],
        compiler_params=pltpu.CompilerParams(
            collective_id=0, has_side_effects=True, vmem_limit_bytes=40 * 1024 * 1024
        ),
    )(*[pltpu.with_memory_space_constraint(a, pltpu.HBM) for a in (jnp.swapaxes(raw_weight, 0, 1), inputs, cotangent)])
    dx, dw = pl.pallas_call(
        hand_over,
        out_shape=(jax.ShapeDtypeStruct(dx.shape, bf16), jax.ShapeDtypeStruct(dw.shape, f32)),
        in_specs=[pl.BlockSpec(memory_space=pltpu.VMEM)] * 2,
        out_specs=[pl.BlockSpec(memory_space=pl.ANY)] * 2,
        scratch_shapes=[dma((2,))],
    )(*[pltpu.with_memory_space_constraint(a, pltpu.VMEM) for a in (dx, dw)])
    return dx, jnp.swapaxes(dw, 0, 1)


def solution(mesh):
    in_specs = (P(("gx", "gy"), None, None), P("gx", "gy", "gz", None), P("gx", "gy", "gz", None))
    out_specs = (P("gx", "gy", "gz", None), P(("gx", "gy"), None, None))
    return jax.shard_map(
        on_device, mesh=mesh, in_specs=in_specs, out_specs=out_specs, check_vma=False
    )
```

```python
import functools

import jax
import jax.numpy as jnp
from jax import lax
from jax.experimental import pallas as pl
from jax.experimental.pallas import tpu as pltpu
from jax.sharding import PartitionSpec as P

var_eps = 1e-05
norm_eps = 1e-06
clip_norm = 600.0

f32 = jnp.float32
bf16 = jnp.bfloat16
MESH = pl.DeviceIdType.MESH

C = 128
LX, LY, LZ = 8, 16, 16
CELLS = LX * LY * LZ
PITCH = 32
FAN = 27 * C

TAPS = [(t // 9, t // 3 % 3, t % 3) for t in range(27)]
CHUNKS = ((0, 2), (2, 4), (4, 7))
DIRECTIONS = [
    (dx, dy, dz)
    for dz in (-1, 1, 0)
    for dx in (0, -1, 1)
    for dy in (0, -1, 1)
    if (dx, dy, dz) != (0, 0, 0)
]


def body(raw_hbm, x_hbm, cot_hbm, dx_ref, dw_ref, raw_ref, x_ref, cot_ref,
         full, pad, zface, zedge, zpoint, zhalo, zcorner, zdot, plane, turned, xf, xt, xy, xz, grad, land_x, land_y, land_c,
         raws, mine_raw, part, norm, w, wt, part_dx, own, psend, precv, spread, r1, red, comp, r2, rows, gath, nat, mine_std, stat,
         ls, hr, wr, dr, ours, got, sent):
    gx, gy, gz = lax.axis_index("gx"), lax.axis_index("gy"), lax.axis_index("gz")
    def div(a, n):
        return lax.div(a, jnp.int32(n))

    def mod(a, n):
        return lax.rem(a, jnp.int32(n))

    z_lo, core = div(gx, 2), mod(gx, 2)
    z_hi, x = div(gz, 4), mod(gz, 4)
    z = z_hi * 4 + z_lo
    mine = gy * 4 + x
    early_tap, late_tap = 2 - 2 * z_hi, 2 * z_hi
    early_side, late_side = z_hi, 1 - z_hi
    full2 = full.reshape(11 * 18 * PITCH, C)

    def dev(a, b, c):
        return (a, b, c)

    def ring(step):
        zz = mod(z + step, 8)
        return mod(zz, 4), div(zz, 4)

    spots = [ring(step) for step in range(8)] + [ring(2 + 4 * core), (mod(z_lo + 2, 4), z_hi)]
    at_gz = [hi * 4 + x for _, hi in spots]
    at_gx = [[lo * 2 + core, lo * 2 + 1 - core] for lo, _ in spots]
    at_gy = [gy] + [mod(gy + k, 4) for k in range(1, 4)]
    at_x = [x] + [mod(x + k, 4) for k in range(1, 4)]
    x_gz = [gz] + [z_hi * 4 + at_x[k] for k in range(1, 4)]

    def chip_peer(step):
        return dev(at_gx[step][0], gy, at_gz[step])

    def gy_peer(k):
        return dev(gx, at_gy[k], gz)

    def x_peer(k):
        return dev(gx, gy, x_gz[k])

    def xy_peer(k):
        return dev(gx, at_gy[k // 4], x_gz[k % 4])

    z_peer = chip_peer
    def plane_peer(k, step):
        return dev(at_gx[step][k // 4], at_gy[k % 4], at_gz[step])

    def to_plane(send):
        for step in (9, 1, 7, 0):
            for k in range(1 if step == 0 else 0, 8):
                send(plane_peer(k, step))

    partner = dev(gx + 1 - 2 * core, gy, gz)

    def remote(src, dst, recv, device):
        return pltpu.make_async_remote_copy(
            src_ref=src, dst_ref=dst, send_sem=sent.at[0], recv_sem=recv, device_id=device, device_id_type=MESH
        )

    def rows_wait(n, sem):
        view = full2.at[pl.ds(0, n)]
        pltpu.make_async_copy(view, view, sem).wait()

    def drain(ref, sem):
        pltpu.make_async_copy(ref, ref, sem).wait()

    def exists(axis_index, last, step):
        if step == 0:
            return None
        return axis_index > 0 if step < 0 else axis_index < last

    def count(axis_index, last):
        return (axis_index > 0).astype(jnp.int32) + (axis_index < last).astype(jnp.int32)

    def present(d):
        tests = [exists(gx, 7, d[0]), exists(gy, 3, d[1]), exists(gz, 7, d[2])]
        tests = [t for t in tests if t is not None]
        out = tests[0]
        for t in tests[1:]:
            out = jnp.logical_and(out, t)
        return out

    loads = [
        pltpu.make_async_copy(a, b, ls.at[n])
        for n, (a, b) in enumerate(((cot_hbm, cot_ref), (raw_hbm, raw_ref), (x_hbm, x_ref)))
    ]
    for load in loads:
        load.start()

    barrier = pltpu.get_barrier_semaphore()

    def greet(device):
        pl.semaphore_signal(barrier, inc=1, device_id=device, device_id_type=MESH)

    wide = [d for d in DIRECTIONS if d[2] != 0]
    greeted = jnp.int32(0)
    for d in wide:
        there = present(d)

        @pl.when(there)
        def _(d=d):
            greet(dev(gx + d[0], gy + d[1], gz + d[2]))

        greeted = greeted + there.astype(jnp.int32)
    greet(z_peer(2))
    greet(z_peer(6))
    for k in (10, 11, 9, 6, 14, 5, 7, 13, 15, 1, 2, 3):
        greet(xy_peer(k))
    to_plane(greet)

    loads[0].wait()

    def fill(i, _):
        slab = cot_ref[i]
        pad[1, i + 1, 1 : LY + 1] = slab
        full[i + 1, 1 : LY + 1, 8 : 8 + LZ, :] = slab.astype(f32)
        return 0

    lax.fori_loop(0, LX, fill, 0)

    def faces(i, _):
        for s, zr in ((0, 8), (1, 8 + LZ - 1)):
            zface[s, i] = full2[pl.ds(((i + 1) * 18 + 1) * PITCH + zr, LY, stride=PITCH), :].astype(bf16)
        return 0

    lax.fori_loop(0, LX, faces, 0)
    for s, zr in ((0, 8), (1, 8 + LZ - 1)):
        for e, yr in ((0, 1), (1, LY)):
            for i in range(LX):
                at = ((i + 1) * 18 + yr) * PITCH + zr
                plane[s, e, i : i + 1, :] = full2[at : at + 1, :]
            zedge[s, e] = plane[s, e, 0:LX, :].astype(bf16)
            zpoint[s, e, 0] = plane[s, e, 0:1, :]
            zpoint[s, e, 1] = plane[s, e, LX - 1 : LX, :]
    loads[1].wait()
    raws[gy] = raw_ref[...]
    first = jnp.zeros((4, C), f32)
    second = jnp.zeros((4, C), f32)
    for t in range(27):
        v = raw_ref[t]
        first = first + v
        second = second + v * v
    part[gx * 4 + gy, 0:1, :] = jnp.sum(first, axis=0, keepdims=True)
    part[gx * 4 + gy, 1:2, :] = jnp.sum(second, axis=0, keepdims=True)

    pl.semaphore_wait(barrier, greeted + (2 + 12 + 31))

    def halo_copy(d):
        dx, dy, dz = d
        xs, xd = (None, None) if dx == 0 else ((0, 1) if dx < 0 else (LX - 1, 0))
        ys, yd = (None, None) if dy == 0 else ((0, 1) if dy < 0 else (LY - 1, 0))
        if dz == 0:
            if dy == 0:
                src, dst = cot_ref.at[xs], land_x.at[xd]
            elif dx == 0:
                src, dst = cot_ref.at[:, ys], land_y.at[yd]
            else:
                src, dst = cot_ref.at[xs, ys], land_c.at[xd, yd]
        else:
            s = 0 if dz < 0 else 1
            r = 1 - s
            if dy == 0:
                if dx == 0:
                    src, dst = zface.at[s], zhalo.at[r, pl.ds(1, LX)]
                else:
                    src, dst = zface.at[s, xs], zhalo.at[r, 9 * xd]
            else:
                e = 0 if dy < 0 else 1
                if dx == 0:
                    src, dst = zedge.at[s, e], zcorner.at[r, 1 - e]
                elif dx < 0:
                    src, dst = zpoint.at[s, e, 0], zdot.at[r, 1 - e, 1]
                else:
                    src, dst = zpoint.at[s, e, 1], zdot.at[r, 1 - e, 0]
        return remote(src, dst, hr.at[0 if dz == 0 else (2 if dz < 0 else 1)], dev(gx + dx, gy + dy, gz + dz))

    def send_part(device):
        here = part.at[gx * 4 + gy]
        remote(here, here, wr.at[1], device).start()

    busy = jnp.logical_or(gz == 3, gz == 4)

    def large(d):
        return d[1] == 0 and d[2] == 0

    for d in DIRECTIONS:
        there = present(d)
        if large(d):
            there = jnp.logical_and(there, jnp.logical_not(busy))

        @pl.when(there)
        def _(d=d):
            halo_copy(d).start()

    near_x, near_y, near_z = count(gx, 7), count(gy, 3), count(gz, 7)

    def flat_rows(nx, ny):
        return 128 * nx + 64 * ny + 8 * nx * ny

    def wide_rows(nx, ny):
        return 64 + 8 * nx + 4 * ny + nx * ny

    def by_neighbours(rows, sem):
        for nx in (1, 2):
            for ny in (1, 2):

                @pl.when(jnp.logical_and(near_x == nx, near_y == ny))
                def _(nx=nx, ny=ny):
                    rows_wait(rows(nx, ny), sem)

    def wide_wait(late):
        for half in (0, 1):
            there = z_hi == half
            if not late:
                there = jnp.logical_and(there, near_z == 2)

            @pl.when(there)
            def _(half=half):
                by_neighbours(wide_rows, hr.at[1 + (1 - half if late else half)])

    for k in (2, 1, 3):
        remote(raw_ref, raws.at[gy], wr.at[0], gy_peer(k)).start()
    to_plane(send_part)

    tile = jnp.zeros((LZ, C), bf16)

    for c in range(3):
        for i in (0, 9):
            for j in range(18):
                pad[c, i, j] = tile
        for i in range(1, 9):
            pad[c, i, 0] = tile
            pad[c, i, 17] = tile

    for k, x_there in ((0, gx > 0), (1, gx < 7)):

        @pl.when(jnp.logical_not(x_there))
        def _(k=k):
            for j in range(LY):
                land_x[k, j] = tile

        for e, y_there in ((0, gy > 0), (1, gy < 3)):

            @pl.when(jnp.logical_not(jnp.logical_and(x_there, y_there)))
            def _(k=k, e=e):
                land_c[k, e] = tile

    for e, y_there in ((0, gy > 0), (1, gy < 3)):

        @pl.when(jnp.logical_not(y_there))
        def _(e=e):
            for i in range(LX):
                land_y[e, i] = tile

    for r, z_there in ((0, gz > 0), (1, gz < 7)):

        @pl.when(jnp.logical_not(z_there))
        def _(r=r):
            for i in range(10):
                zhalo[r, i] = tile

        for k, x_there in ((0, gx > 0), (1, gx < 7)):

            @pl.when(jnp.logical_and(z_there, jnp.logical_not(x_there)))
            def _(r=r, k=k):
                zhalo[r, 9 * k] = tile

        for e, y_there in ((0, gy > 0), (1, gy < 3)):
            both = jnp.logical_and(z_there, y_there)

            @pl.when(jnp.logical_not(both))
            def _(r=r, e=e):
                zcorner[r, e] = jnp.zeros((8, C), bf16)

            for k, x_there in ((0, gx > 0), (1, gx < 7)):

                @pl.when(jnp.logical_not(jnp.logical_and(both, x_there)))
                def _(r=r, e=e, k=k):
                    zdot[r, e, k] = jnp.zeros((1, C), f32)

    for i in range(10):
        for zr in (7, 8 + LZ):
            full2[pl.ds(i * 18 * PITCH + zr, 18, stride=PITCH), :] = jnp.zeros((18, C), f32)

    def shift(i, _):
        pad[0, i] = full[i, :, 9 : 9 + LZ, :].astype(bf16)
        pad[2, i] = full[i, :, 7 : 7 + LZ, :].astype(bf16)
        return 0

    def shift_inside(i, _):
        inside = slice(1, LY + 1)
        pad[0, i, inside] = full[i, inside, 9 : 9 + LZ, :].astype(bf16)
        pad[2, i, inside] = full[i, inside, 7 : 7 + LZ, :].astype(bf16)
        return 0

    lax.fori_loop(1, LX + 1, shift_inside, 0)
    loads[2].wait()
    m = lax.broadcasted_iota(jnp.int32, (C, C), 0)
    col = lax.broadcasted_iota(jnp.int32, (C, C), 1)
    want = (m % 4) * 32 + (m // 4 + 16 * core) % 32
    order = jnp.where(col == want, 1.0, 0.0).astype(bf16)
    for j in range(4):
        xt[:, j * 512 : (j + 1) * 512] = lax.dot_general(
            order,
            x_ref[2 * j : 2 * j + 2].reshape(512, C),
            (((1,), (1,)), ((), ())),
            preferred_element_type=f32,
        ).astype(bf16)

    for d in DIRECTIONS:
        if large(d):

            @pl.when(jnp.logical_and(present(d), busy))
            def _(d=d):
                halo_copy(d).start()

    def widen(i, _):
        xf[pl.ds(pl.multiple_of(i * LY * LZ, LY * LZ), LY * LZ), :] = x_ref[i].reshape(LY * LZ, C).astype(f32)
        return 0

    lax.fori_loop(0, LX, widen, 0)
    def by_channel(cells):
        return lax.dot_general(order, cells, (((1,), (1,)), ((), ())), preferred_element_type=f32).astype(bf16)

    for n, e in ((0, 0), (1, LZ - 1)):
        xy[n] = by_channel(x_ref[:, e].reshape(LX * LZ, C))
        xz[n] = by_channel(xf[pl.ds(e, LX * LY, stride=LZ), :].astype(bf16))

    def tap_of(p):
        return p % 9 // 3, p % 3, (1, early_tap, late_tap)[p // 9]

    for p in range(0, 27, 2):
        views = []
        for t in range(p, min(p + 2, 27)):
            a, b, c = tap_of(t)
            views.append(pad[c, 2 - a : 2 - a + LX, 2 - b : 2 - b + LY].reshape(CELLS, C))
        v = jnp.concatenate(views, axis=1) if len(views) == 2 else views[0]
        o = jnp.dot(xt[...], v, preferred_element_type=f32)
        for n in range(len(views)):
            grad[p + n] = o[:, n * C : (n + 1) * C]
    grad[27] = jnp.zeros((C, C), f32)

    def add_side(lhs, taps, view):
        o = jnp.dot(lhs, jnp.concatenate([view(p) for p in taps], axis=1), preferred_element_type=f32)
        for n, p in enumerate(taps):
            grad[p] += o[:, n * C : (n + 1) * C]

    def quad(q):
        outs = [grad[p] for p in range(4 * q, 4 * q + 4)]
        low = lax.broadcasted_iota(jnp.int32, (16, 8, C), 1) < 4
        pieces = [[], []]
        for h in range(2):
            one = outs[2 * h].reshape(16, 8, C)
            two = outs[2 * h + 1].reshape(16, 8, C)
            pieces[0].append(jnp.where(low, one, pltpu.roll(two, 4, 1)))
            pieces[1].append(jnp.where(low, pltpu.roll(one, 4, 1), two))
        for e in range(2):
            t = jnp.concatenate(pieces[e], axis=1)
            for j in range(8):
                own[q, 2 * j + e] = t[j]
                psend[q, 2 * j + e] = t[8 + j].astype(bf16)

    def quads(n):
        lo, hi = CHUNKS[n]
        for q in range(lo, hi):
            quad(q)
        some = pl.ds(lo, hi - lo)
        remote(psend.at[some], precv.at[some], dr.at[n], partner).start()

    def spread_chunk(n):
        lo, hi = CHUNKS[n]
        drain(precv.at[pl.ds(lo, hi - lo)], dr.at[n])
        for q in range(lo, hi):
            spread[:, q] = (own[q] + precv[q].astype(f32)).astype(bf16)

        for k in (10, 11, 9, 6, 14, 2, 8, 5, 7, 13, 15, 1, 3, 4, 12):
            remote(
                spread.at[at_gy[k // 4] * 4 + at_x[k % 4], pl.ds(lo, hi - lo)],
                r1.at[k - 1, pl.ds(lo, hi - lo)],
                got.at[1],
                xy_peer(k),
            ).start()

    by_neighbours(flat_rows, hr.at[0])
    for e, yr in ((0, 0), (1, LY + 1)):
        face = land_y[e]
        pad[1, 1 : LX + 1, yr] = face
        full[1 : LX + 1, yr, 8 : 8 + LZ, :] = face.astype(f32)
        pad[0, 1 : LX + 1, yr] = full[1 : LX + 1, yr, 9 : 9 + LZ, :].astype(bf16)
        pad[2, 1 : LX + 1, yr] = full[1 : LX + 1, yr, 7 : 7 + LZ, :].astype(bf16)

        def view_y(p, yr=yr):
            a, _, c = tap_of(p)
            return pad[c, 2 - a : 2 - a + LX, yr].reshape(LX * LZ, C)

        add_side(xy[e], [p for p in range(27) if p % 3 == (2 if e == 0 else 0)], view_y)
    for k, xr in ((0, 0), (1, LX + 1)):
        pad[1, xr, 1 : LY + 1] = land_x[k]
        full[xr, 1 : LY + 1, 8 : 8 + LZ, :] = land_x[k].astype(f32)
        for e, yr in ((0, 0), (1, LY + 1)):
            pad[1, xr, yr] = land_c[k, e]
            full[xr, yr, 8 : 8 + LZ, :] = land_c[k, e].astype(f32)
        shift(xr, 0)

        def view_x(p, xr=xr):
            _, b, c = tap_of(p)
            return pad[c, xr, 2 - b : 2 - b + LY].reshape(LY * LZ, C)

        cells = LY * LZ
        lhs = xt[:, :cells] if k == 0 else xt[:, CELLS - cells :]
        add_side(lhs, [p for p in range(27) if p % 9 // 3 == (2 if k == 0 else 0)], view_x)
    quads(0)
    def lay_out(side):
        edges = [zcorner[side, e].astype(f32) for e in range(2)]
        for i in range(10):
            plane[side, i, 8 : 8 + LY, :] = zhalo[side, i].astype(f32)
            for e, yr in ((0, 7), (1, 8 + LY)):
                if 0 < i < 9:
                    plane[side, i, yr : yr + 1, :] = edges[e][i - 1 : i]
                else:
                    plane[side, i, yr : yr + 1, :] = zdot[side, e, i // 9]
        for i in range(10):
            turned[1, i] = zhalo[side, i]
            for b in (0, 2):
                turned[b, i] = plane[side, i, 9 - b : 9 - b + LY, :].astype(bf16)

    def put_in(side):
        zr = 7 + 17 * side

        def put(i, _):
            full2[pl.ds(i * 18 * PITCH + zr, 18, stride=PITCH), :] = plane[side, i, 7 : 7 + 18, :]
            return 0

        lax.fori_loop(0, 10, put, 0)

    def view_z(p):
        a, b, _ = tap_of(p)
        return turned[b, 2 - a : 2 - a + LX].reshape(LX * LY, C)

    wide_wait(False)
    lay_out(early_side)
    add_side(xz[early_side], range(9, 18), view_z)
    quads(1)
    far = jnp.logical_or(gz == 3, gz == 4)

    halves = (slice(0, 14 * C), slice(14 * C, 27 * C))

    def slab(g, h):
        return w.at[pl.ds(pl.multiple_of(g * 16, 16), 16), halves[h]]

    def filter_rows():
        drain(part.at[pl.ds(0, 31)], wr.at[1])
        drain(raws.at[pl.ds(0, 3)], wr.at[0])
        total = part[0]
        for j in range(1, 32):
            total = total + part[j]
        mean = total[0:1] / FAN
        var = total[1:2] / FAN - mean * mean
        inv = lax.rsqrt(var + var_eps)
        norm[0:1, :] = mean
        norm[1:2, :] = var
        norm[2:3, :] = inv
        for t in range(27):
            for j in range(4):
                mine_raw[t, 4 * j : 4 * j + 4, :] = raws[j, t]
        mine_rows = pl.ds(pl.multiple_of(gx * 16, 16), 16)
        for p in range(27):
            a, b, c = TAPS[p]
            t = 9 * a + 3 * b + c
            w[mine_rows, p * C : (p + 1) * C] = ((mine_raw[t] - mean) * inv).astype(bf16)
        for t in range(27):
            mine_std[4 * t : 4 * t + 4, :] = (raw_ref[t] - mean) * inv
        for h in range(2):
            for step in (8, 1, 7):
                remote(slab(gx, h), slab(gx, h), wr.at[2 + h], chip_peer(step)).start()
        for h in range(2):
            remote(slab(gx, h), slab(gx, h), ours.at[h], partner).start()

    def finish():
        wide_wait(True)
        lay_out(late_side)
        add_side(xz[late_side], range(18, 27), view_z)
        quads(2)

    @pl.when(jnp.logical_not(far))
    def _():
        finish()

    spread_chunk(0)
    spread_chunk(1)

    @pl.when(far)
    def _():
        filter_rows()
        finish()

    spread_chunk(2)

    @pl.when(jnp.logical_not(far))
    def _():
        filter_rows()

    mean, var, inv = norm[0:1, :], norm[1:2, :], norm[2:3, :]

    def hand_on(h):
        drain(w.at[pl.ds(0, 48), halves[h]], wr.at[2 + h])
        for k in (1, 2, 3):
            g = at_gx[k][0]
            remote(slab(g, h), slab(g, h), ours.at[h], partner).start()

    def take_over(h):
        drain(w.at[pl.ds(0, 64), halves[h]], ours.at[h])
        for p in range(14 * h, 14 + 13 * h):
            wt[p * C : (p + 1) * C, :] = w[:, p * C : (p + 1) * C].T

    def input_grad(h, lo, hi):
        def one(i, _):
            views = []
            for a, b, c in TAPS[14 * h : 14 + 13 * h]:
                views.append(pad[c, pl.ds(2 * i + 2 - a, 2), 2 - b : 2 - b + LY].reshape(2 * LY * LZ, C))
            out = jnp.dot(jnp.concatenate(views, axis=1), wt[halves[h], :], preferred_element_type=f32)
            if h == 0:
                part_dx[i] = out
            else:
                dx_ref[pl.ds(2 * i, 2)] = (part_dx[i] + out).astype(bf16).reshape(2, LY, LZ, C)
            return 0

        lax.fori_loop(lo, hi, one, 0)

    put_in(0)
    put_in(1)
    lax.fori_loop(0, 10, shift, 0)
    hand_on(0)
    drain(r1, got.at[1])
    for q in range(7):
        acc = own[q, mine] + precv[q, mine].astype(f32)
        for k in range(15):
            acc = acc + r1[k, q].astype(f32)
        red[q * 16 : (q + 1) * 16, :] = acc
    for j in range(4):
        for n, start in enumerate((0, 72 - 36 * z_hi, 36 + 36 * z_hi)):
            comp[j, 9 * n : 9 * n + 9, :] = red[pl.ds(start + j, 9, stride=4), :]
        comp[j, 27:32, :] = jnp.zeros((5, C), f32)
        rows[j] = comp[j].astype(bf16)
    r2[z] = rows[z_lo]

    for k in (4, 3, 5, 2, 6, 1, 7):
        remote(rows.at[spots[k][0]], r2.at[z], got.at[2], z_peer(k)).start()

    take_over(0)
    input_grad(0, 0, 4)
    hand_on(1)
    drain(r2.at[pl.ds(0, 7)], got.at[2])
    acc = r2[0].astype(f32)
    for j in range(1, 8):
        acc = acc + r2[j].astype(f32)
    gath[x] = acc

    for k in (2, 1, 3):
        remote(gath.at[x], gath.at[x], got.at[3], x_peer(k)).start()
    take_over(1)
    input_grad(1, 0, 2)

    drain(gath.at[pl.ds(0, 3)], got.at[3])
    for r in range(4):
        for n, c in enumerate((1, 0, 2)):
            nat[pl.ds(4 * c + r, 9, stride=12), :] = gath[r, n * 9 : n * 9 + 9, :]
    g = nat[0:108, :]
    std = mine_std[0:108, :]
    here = gx * 4 + gy
    stat[here, 0:1, :] = jnp.sum(g, axis=0, keepdims=True)
    stat[here, 1:2, :] = jnp.sum(g * std, axis=0, keepdims=True)
    stat[here, 2:3, :] = jnp.sum(g * g, axis=0, keepdims=True)
    stat[here, 3:4, :] = jnp.zeros((1, C), f32)

    def send_stat(device):
        remote(stat.at[here], stat.at[here], got.at[4], device).start()

    to_plane(send_stat)
    input_grad(1, 2, 4)
    drain(stat.at[pl.ds(0, 31)], got.at[4])
    total = stat[0]
    for j in range(1, 32):
        total = total + stat[j]
    sum_grad, sum_cross, sum_square = total[0:1], total[1:2], total[2:3]
    mean_grad = sum_grad / FAN
    mean_cross = sum_cross / FAN
    per_output = sum_square - 2.0 * mean_grad * sum_grad - 2.0 * mean_cross * sum_cross
    per_output = (
        per_output + FAN * mean_grad * mean_grad + FAN * mean_cross * mean_cross * var / (var + var_eps)
    )
    square_sum = jnp.sum(inv * inv * per_output, axis=1, keepdims=True)
    scale = jnp.minimum(1.0, clip_norm * lax.rsqrt(square_sum + norm_eps))
    factor = inv * scale
    for t in range(27):
        g = nat[4 * t : 4 * t + 4, :]
        dw_ref[t] = factor * (g - mean_grad - mine_std[4 * t : 4 * t + 4, :] * mean_cross)

    always = (3 * 27 * 4 * C + 31 * 2 * C + 31 * 4 * C + 3 * 32 * C) * 4 + (
        7 * 16 * 27 * C + 7 * 256 * C + 15 * 112 * C + 7 * 32 * C
    ) * 2
    for nz in (1, 2):

        @pl.when(near_z == nz)
        def _(nz=nz):
            by_neighbours(
                lambda nx, ny: flat_rows(nx, ny) + nz * wide_rows(nx, ny) + always // (4 * C), sent.at[0]
            )


def hand_over(dx_in, dw_in, dx_out, dw_out, sems):
    copies = [
        pltpu.make_async_copy(a, b, sems.at[n]) for n, (a, b) in enumerate(((dx_in, dx_out), (dw_in, dw_out)))
    ]
    for copy in copies:
        copy.start()
    for copy in copies:
        copy.wait()


def on_device(raw_weight, inputs, cotangent):
    dma = pltpu.SemaphoreType.DMA
    vmem = pltpu.VMEM
    dx, dw = pl.pallas_call(
        body,
        out_shape=(
            pltpu.VMEM(inputs.shape, bf16),
            pltpu.VMEM((27, 4, C), f32),
        ),
        in_specs=[pl.BlockSpec(memory_space=pltpu.HBM)] * 3,
        out_specs=[pl.BlockSpec(memory_space=pltpu.VMEM)] * 2,
        scratch_shapes=[
            vmem((27, 4, C), f32),
            vmem((LX, LY, LZ, C), bf16),
            vmem((LX, LY, LZ, C), bf16),
            vmem((11, 18, PITCH, C), f32),
            vmem((3, 10, 18, LZ, C), bf16),
            vmem((2, LX, LY, C), bf16),
            vmem((2, 2, 8, C), bf16),
            vmem((2, 2, 2, 1, C), f32),
            vmem((2, 10, LY, C), bf16),
            vmem((2, 2, 8, C), bf16),
            vmem((2, 2, 2, 1, C), f32),
            vmem((2, 10, 32, C), f32),
            vmem((3, 10, LY, C), bf16),
            vmem((CELLS + LZ, C), f32),
            vmem((C, CELLS), bf16),
            vmem((2, C, C), bf16),
            vmem((2, C, C), bf16),
            vmem((28, C, C), f32),
            vmem((2, LY, LZ, C), bf16),
            vmem((2, LX, LZ, C), bf16),
            vmem((2, 2, LZ, C), bf16),
            vmem((4, 27, 4, C), f32),
            vmem((27, 16, C), f32),
            vmem((32, 2, C), f32),
            vmem((8, C), f32),
            vmem((C, 27 * C), bf16),
            vmem((27 * C, C), bf16),
            vmem((LX // 2, 2 * LY * LZ, C), f32),
            vmem((7, 16, 16, C), f32),
            vmem((7, 16, 16, C), bf16),
            vmem((7, 16, 16, C), bf16),
            vmem((16, 7, 16, C), bf16),
            vmem((15, 7, 16, C), bf16),
            vmem((112, C), f32),
            vmem((4, 32, C), f32),
            vmem((8, 32, C), bf16),
            vmem((4, 32, C), bf16),
            vmem((4, 32, C), f32),
            vmem((120, C), f32),
            vmem((112, C), f32),
            vmem((32, 4, C), f32),
            dma((3,)),
            dma((3,)),
            dma((4,)),
            dma((3,)),
            dma((2,)),
            dma((5,)),
            dma((1,)),
        ],
        compiler_params=pltpu.CompilerParams(
            collective_id=0, has_side_effects=True, vmem_limit_bytes=40 * 1024 * 1024
        ),
    )(*[pltpu.with_memory_space_constraint(a, pltpu.HBM) for a in (jnp.swapaxes(raw_weight, 0, 1), inputs, cotangent)])
    dx, dw = pl.pallas_call(
        hand_over,
        out_shape=(jax.ShapeDtypeStruct(dx.shape, bf16), jax.ShapeDtypeStruct(dw.shape, f32)),
        in_specs=[pl.BlockSpec(memory_space=pltpu.VMEM)] * 2,
        out_specs=[pl.BlockSpec(memory_space=pl.ANY)] * 2,
        scratch_shapes=[dma((2,))],
    )(*[pltpu.with_memory_space_constraint(a, pltpu.VMEM) for a in (dx, dw)])
    return dx, jnp.swapaxes(dw, 0, 1)


def solution(mesh):
    in_specs = (P(("gx", "gy"), None, None), P("gx", "gy", "gz", None), P("gx", "gy", "gz", None))
    out_specs = (P("gx", "gy", "gz", None), P(("gx", "gy"), None, None))
    return jax.shard_map(
        on_device, mesh=mesh, in_specs=in_specs, out_specs=out_specs, check_vma=False
    )
```

```python
import functools

import jax
import jax.numpy as jnp
from jax import lax
from jax.experimental import pallas as pl
from jax.experimental.pallas import tpu as pltpu
from jax.sharding import PartitionSpec as P

var_eps = 1e-05
norm_eps = 1e-06
clip_norm = 600.0

f32 = jnp.float32
bf16 = jnp.bfloat16
MESH = pl.DeviceIdType.MESH

C = 128
LX, LY, LZ = 8, 16, 16
CELLS = LX * LY * LZ
PITCH = 32
FAN = 27 * C

TAPS = [(t // 9, t // 3 % 3, t % 3) for t in range(27)]
CHUNKS = ((0, 2), (2, 4), (4, 7))
DIRECTIONS = [
    (dx, dy, dz)
    for dz in (-1, 1, 0)
    for dx in (0, -1, 1)
    for dy in (0, -1, 1)
    if (dx, dy, dz) != (0, 0, 0)
]


def body(raw_hbm, x_hbm, cot_hbm, dx_ref, dw_ref, raw_ref, x_ref, cot_ref,
         full, pad, zface, zedge, zpoint, zhalo, zcorner, zdot, plane, turned, xf, xt, xy, xz, grad, land_x, land_y, land_c,
         raws, mine_raw, part, norm, w, wt, part_dx, own, psend, precv, spread, r1, red, comp, r2, rows, gath, nat, mine_std, stat,
         ls, hr, wr, dr, ours, got, sent):
    gx, gy, gz = lax.axis_index("gx"), lax.axis_index("gy"), lax.axis_index("gz")
    def div(a, n):
        return lax.div(a, jnp.int32(n))

    def mod(a, n):
        return lax.rem(a, jnp.int32(n))

    z_lo, core = div(gx, 2), mod(gx, 2)
    z_hi, x = div(gz, 4), mod(gz, 4)
    z = z_hi * 4 + z_lo
    mine = gy * 4 + x
    early_tap, late_tap = 2 - 2 * z_hi, 2 * z_hi
    early_side, late_side = z_hi, 1 - z_hi
    full2 = full.reshape(11 * 18 * PITCH, C)

    def dev(a, b, c):
        return (a, b, c)

    def ring(step):
        zz = mod(z + step, 8)
        return mod(zz, 4), div(zz, 4)

    spots = [ring(step) for step in range(8)] + [ring(2 + 4 * core), (mod(z_lo + 2, 4), z_hi)]
    at_gz = [hi * 4 + x for _, hi in spots]
    at_gx = [[lo * 2 + core, lo * 2 + 1 - core] for lo, _ in spots]
    at_gy = [gy] + [mod(gy + k, 4) for k in range(1, 4)]
    at_x = [x] + [mod(x + k, 4) for k in range(1, 4)]
    x_gz = [gz] + [z_hi * 4 + at_x[k] for k in range(1, 4)]

    def chip_peer(step):
        return dev(at_gx[step][0], gy, at_gz[step])

    def gy_peer(k):
        return dev(gx, at_gy[k], gz)

    def x_peer(k):
        return dev(gx, gy, x_gz[k])

    def xy_peer(k):
        return dev(gx, at_gy[k // 4], x_gz[k % 4])

    z_peer = chip_peer
    def plane_peer(k, step):
        return dev(at_gx[step][k // 4], at_gy[k % 4], at_gz[step])

    def to_plane(send):
        for step in (9, 1, 7, 0):
            for k in range(1 if step == 0 else 0, 8):
                send(plane_peer(k, step))

    partner = dev(gx + 1 - 2 * core, gy, gz)

    def remote(src, dst, recv, device):
        return pltpu.make_async_remote_copy(
            src_ref=src, dst_ref=dst, send_sem=sent.at[0], recv_sem=recv, device_id=device, device_id_type=MESH
        )

    def rows_wait(n, sem):
        view = full2.at[pl.ds(0, n)]
        pltpu.make_async_copy(view, view, sem).wait()

    def drain(ref, sem):
        pltpu.make_async_copy(ref, ref, sem).wait()

    def exists(axis_index, last, step):
        if step == 0:
            return None
        return axis_index > 0 if step < 0 else axis_index < last

    def count(axis_index, last):
        return (axis_index > 0).astype(jnp.int32) + (axis_index < last).astype(jnp.int32)

    def present(d):
        tests = [exists(gx, 7, d[0]), exists(gy, 3, d[1]), exists(gz, 7, d[2])]
        tests = [t for t in tests if t is not None]
        out = tests[0]
        for t in tests[1:]:
            out = jnp.logical_and(out, t)
        return out

    loads = [
        pltpu.make_async_copy(a, b, ls.at[n])
        for n, (a, b) in enumerate(((cot_hbm, cot_ref), (raw_hbm, raw_ref), (x_hbm, x_ref)))
    ]
    for load in loads:
        load.start()

    barrier = pltpu.get_barrier_semaphore()

    def greet(device):
        pl.semaphore_signal(barrier, inc=1, device_id=device, device_id_type=MESH)

    wide = [d for d in DIRECTIONS if d[2] != 0]
    greeted = jnp.int32(0)
    for d in wide:
        there = present(d)

        @pl.when(there)
        def _(d=d):
            greet(dev(gx + d[0], gy + d[1], gz + d[2]))

        greeted = greeted + there.astype(jnp.int32)
    greet(z_peer(2))
    greet(z_peer(6))
    for k in (10, 11, 9, 6, 14, 5, 7, 13, 15, 1, 2, 3):
        greet(xy_peer(k))
    to_plane(greet)

    loads[0].wait()

    def fill(i, _):
        slab = cot_ref[i]
        pad[1, i + 1, 1 : LY + 1] = slab
        full[i + 1, 1 : LY + 1, 8 : 8 + LZ, :] = slab.astype(f32)
        return 0

    lax.fori_loop(0, LX, fill, 0)

    def faces(i, _):
        for s, zr in ((0, 8), (1, 8 + LZ - 1)):
            zface[s, i] = full2[pl.ds(((i + 1) * 18 + 1) * PITCH + zr, LY, stride=PITCH), :].astype(bf16)
        return 0

    lax.fori_loop(0, LX, faces, 0)
    for s, zr in ((0, 8), (1, 8 + LZ - 1)):
        for e, yr in ((0, 1), (1, LY)):
            for i in range(LX):
                at = ((i + 1) * 18 + yr) * PITCH + zr
                plane[s, e, i : i + 1, :] = full2[at : at + 1, :]
            zedge[s, e] = plane[s, e, 0:LX, :].astype(bf16)
            zpoint[s, e, 0] = plane[s, e, 0:1, :]
            zpoint[s, e, 1] = plane[s, e, LX - 1 : LX, :]
    loads[1].wait()
    raws[gy] = raw_ref[...]
    first = jnp.zeros((4, C), f32)
    second = jnp.zeros((4, C), f32)
    for t in range(27):
        v = raw_ref[t]
        first = first + v
        second = second + v * v
    part[gx * 4 + gy, 0:1, :] = jnp.sum(first, axis=0, keepdims=True)
    part[gx * 4 + gy, 1:2, :] = jnp.sum(second, axis=0, keepdims=True)

    pl.semaphore_wait(barrier, greeted + (2 + 12 + 31))

    def halo_copy(d):
        dx, dy, dz = d
        xs, xd = (None, None) if dx == 0 else ((0, 1) if dx < 0 else (LX - 1, 0))
        ys, yd = (None, None) if dy == 0 else ((0, 1) if dy < 0 else (LY - 1, 0))
        if dz == 0:
            if dy == 0:
                src, dst = cot_ref.at[xs], land_x.at[xd]
            elif dx == 0:
                src, dst = cot_ref.at[:, ys], land_y.at[yd]
            else:
                src, dst = cot_ref.at[xs, ys], land_c.at[xd, yd]
        else:
            s = 0 if dz < 0 else 1
            r = 1 - s
            if dy == 0:
                if dx == 0:
                    src, dst = zface.at[s], zhalo.at[r, pl.ds(1, LX)]
                else:
                    src, dst = zface.at[s, xs], zhalo.at[r, 9 * xd]
            else:
                e = 0 if dy < 0 else 1
                if dx == 0:
                    src, dst = zedge.at[s, e], zcorner.at[r, 1 - e]
                elif dx < 0:
                    src, dst = zpoint.at[s, e, 0], zdot.at[r, 1 - e, 1]
                else:
                    src, dst = zpoint.at[s, e, 1], zdot.at[r, 1 - e, 0]
        return remote(src, dst, hr.at[0 if dz == 0 else (2 if dz < 0 else 1)], dev(gx + dx, gy + dy, gz + dz))

    def send_part(device):
        here = part.at[gx * 4 + gy]
        remote(here, here, wr.at[1], device).start()

    busy = jnp.logical_or(gz == 3, gz == 4)

    def large(d):
        return d[1] == 0 and d[2] == 0

    for d in DIRECTIONS:
        there = present(d)
        if large(d):
            there = jnp.logical_and(there, jnp.logical_not(busy))

        @pl.when(there)
        def _(d=d):
            halo_copy(d).start()

    near_x, near_y, near_z = count(gx, 7), count(gy, 3), count(gz, 7)

    def flat_rows(nx, ny):
        return 128 * nx + 64 * ny + 8 * nx * ny

    def wide_rows(nx, ny):
        return 64 + 8 * nx + 4 * ny + nx * ny

    def by_neighbours(rows, sem):
        for nx in (1, 2):
            for ny in (1, 2):

                @pl.when(jnp.logical_and(near_x == nx, near_y == ny))
                def _(nx=nx, ny=ny):
                    rows_wait(rows(nx, ny), sem)

    def wide_wait(late):
        for half in (0, 1):
            there = z_hi == half
            if not late:
                there = jnp.logical_and(there, near_z == 2)

            @pl.when(there)
            def _(half=half):
                by_neighbours(wide_rows, hr.at[1 + (1 - half if late else half)])

    for k in (2, 1, 3):
        remote(raw_ref, raws.at[gy], wr.at[0], gy_peer(k)).start()

    tile = jnp.zeros((LZ, C), bf16)

    for c in range(3):
        for i in (0, 9):
            for j in range(18):
                pad[c, i, j] = tile
        for i in range(1, 9):
            pad[c, i, 0] = tile
            pad[c, i, 17] = tile

    for k, x_there in ((0, gx > 0), (1, gx < 7)):

        @pl.when(jnp.logical_not(x_there))
        def _(k=k):
            for j in range(LY):
                land_x[k, j] = tile

        for e, y_there in ((0, gy > 0), (1, gy < 3)):

            @pl.when(jnp.logical_not(jnp.logical_and(x_there, y_there)))
            def _(k=k, e=e):
                land_c[k, e] = tile

    for e, y_there in ((0, gy > 0), (1, gy < 3)):

        @pl.when(jnp.logical_not(y_there))
        def _(e=e):
            for i in range(LX):
                land_y[e, i] = tile

    for r, z_there in ((0, gz > 0), (1, gz < 7)):

        @pl.when(jnp.logical_not(z_there))
        def _(r=r):
            for i in range(10):
                zhalo[r, i] = tile

        for k, x_there in ((0, gx > 0), (1, gx < 7)):

            @pl.when(jnp.logical_and(z_there, jnp.logical_not(x_there)))
            def _(r=r, k=k):
                zhalo[r, 9 * k] = tile

        for e, y_there in ((0, gy > 0), (1, gy < 3)):
            both = jnp.logical_and(z_there, y_there)

            @pl.when(jnp.logical_not(both))
            def _(r=r, e=e):
                zcorner[r, e] = jnp.zeros((8, C), bf16)

            for k, x_there in ((0, gx > 0), (1, gx < 7)):

                @pl.when(jnp.logical_not(jnp.logical_and(both, x_there)))
                def _(r=r, e=e, k=k):
                    zdot[r, e, k] = jnp.zeros((1, C), f32)

    for i in range(10):
        for zr in (7, 8 + LZ):
            full2[pl.ds(i * 18 * PITCH + zr, 18, stride=PITCH), :] = jnp.zeros((18, C), f32)

    def shift(i, _):
        pad[0, i] = full[i, :, 9 : 9 + LZ, :].astype(bf16)
        pad[2, i] = full[i, :, 7 : 7 + LZ, :].astype(bf16)
        return 0

    def shift_inside(i, _):
        inside = slice(1, LY + 1)
        pad[0, i, inside] = full[i, inside, 9 : 9 + LZ, :].astype(bf16)
        pad[2, i, inside] = full[i, inside, 7 : 7 + LZ, :].astype(bf16)
        return 0

    lax.fori_loop(1, LX + 1, shift_inside, 0)
    loads[2].wait()
    m = lax.broadcasted_iota(jnp.int32, (C, C), 0)
    col = lax.broadcasted_iota(jnp.int32, (C, C), 1)
    want = (m % 4) * 32 + (m // 4 + 16 * core) % 32
    order = jnp.where(col == want, 1.0, 0.0).astype(bf16)
    for j in range(4):
        xt[:, j * 512 : (j + 1) * 512] = lax.dot_general(
            order,
            x_ref[2 * j : 2 * j + 2].reshape(512, C),
            (((1,), (1,)), ((), ())),
            preferred_element_type=f32,
        ).astype(bf16)

    for d in DIRECTIONS:
        if large(d):

            @pl.when(jnp.logical_and(present(d), busy))
            def _(d=d):
                halo_copy(d).start()

    to_plane(send_part)

    def widen(i, _):
        xf[pl.ds(pl.multiple_of(i * LY * LZ, LY * LZ), LY * LZ), :] = x_ref[i].reshape(LY * LZ, C).astype(f32)
        return 0

    lax.fori_loop(0, LX, widen, 0)
    def by_channel(cells):
        return lax.dot_general(order, cells, (((1,), (1,)), ((), ())), preferred_element_type=f32).astype(bf16)

    for n, e in ((0, 0), (1, LZ - 1)):
        xy[n] = by_channel(x_ref[:, e].reshape(LX * LZ, C))
        xz[n] = by_channel(xf[pl.ds(e, LX * LY, stride=LZ), :].astype(bf16))

    def tap_of(p):
        return p % 9 // 3, p % 3, (1, early_tap, late_tap)[p // 9]

    for p in range(0, 27, 2):
        views = []
        for t in range(p, min(p + 2, 27)):
            a, b, c = tap_of(t)
            views.append(pad[c, 2 - a : 2 - a + LX, 2 - b : 2 - b + LY].reshape(CELLS, C))
        v = jnp.concatenate(views, axis=1) if len(views) == 2 else views[0]
        o = jnp.dot(xt[...], v, preferred_element_type=f32)
        for n in range(len(views)):
            grad[p + n] = o[:, n * C : (n + 1) * C]
    grad[27] = jnp.zeros((C, C), f32)

    def add_side(lhs, taps, view):
        o = jnp.dot(lhs, jnp.concatenate([view(p) for p in taps], axis=1), preferred_element_type=f32)
        for n, p in enumerate(taps):
            grad[p] += o[:, n * C : (n + 1) * C]

    def quad(q, late=None):
        outs = [grad[p] for p in range(4 * q, 4 * q + 4)]
        if late is not None:
            for n, p in enumerate(range(4 * q, 4 * q + 4)):
                if 18 <= p < 27:
                    outs[n] = outs[n] + late[:, (p - 18) * C : (p - 17) * C]
        low = lax.broadcasted_iota(jnp.int32, (16, 8, C), 1) < 4
        pieces = [[], []]
        for h in range(2):
            one = outs[2 * h].reshape(16, 8, C)
            two = outs[2 * h + 1].reshape(16, 8, C)
            pieces[0].append(jnp.where(low, one, pltpu.roll(two, 4, 1)))
            pieces[1].append(jnp.where(low, pltpu.roll(one, 4, 1), two))
        for e in range(2):
            t = jnp.concatenate(pieces[e], axis=1)
            for j in range(8):
                own[q, 2 * j + e] = t[j]
                psend[q, 2 * j + e] = t[8 + j].astype(bf16)

    def quads(n, late=None):
        lo, hi = CHUNKS[n]
        for q in range(lo, hi):
            quad(q, late)
        some = pl.ds(lo, hi - lo)
        remote(psend.at[some], precv.at[some], dr.at[n], partner).start()

    def spread_chunk(n):
        lo, hi = CHUNKS[n]
        drain(precv.at[pl.ds(lo, hi - lo)], dr.at[n])
        for q in range(lo, hi):
            spread[:, q] = (own[q] + precv[q].astype(f32)).astype(bf16)

        for k in (10, 11, 9, 6, 14, 2, 8, 5, 7, 13, 15, 1, 3, 4, 12):
            remote(
                spread.at[at_gy[k // 4] * 4 + at_x[k % 4], pl.ds(lo, hi - lo)],
                r1.at[k - 1, pl.ds(lo, hi - lo)],
                got.at[1],
                xy_peer(k),
            ).start()

    by_neighbours(flat_rows, hr.at[0])
    for e, yr in ((0, 0), (1, LY + 1)):
        face = land_y[e]
        pad[1, 1 : LX + 1, yr] = face
        full[1 : LX + 1, yr, 8 : 8 + LZ, :] = face.astype(f32)
        pad[0, 1 : LX + 1, yr] = full[1 : LX + 1, yr, 9 : 9 + LZ, :].astype(bf16)
        pad[2, 1 : LX + 1, yr] = full[1 : LX + 1, yr, 7 : 7 + LZ, :].astype(bf16)

        def view_y(p, yr=yr):
            a, _, c = tap_of(p)
            return pad[c, 2 - a : 2 - a + LX, yr].reshape(LX * LZ, C)

        add_side(xy[e], [p for p in range(27) if p % 3 == (2 if e == 0 else 0)], view_y)
    for k, xr in ((0, 0), (1, LX + 1)):
        pad[1, xr, 1 : LY + 1] = land_x[k]
        full[xr, 1 : LY + 1, 8 : 8 + LZ, :] = land_x[k].astype(f32)
        for e, yr in ((0, 0), (1, LY + 1)):
            pad[1, xr, yr] = land_c[k, e]
            full[xr, yr, 8 : 8 + LZ, :] = land_c[k, e].astype(f32)
        shift(xr, 0)

        def view_x(p, xr=xr):
            _, b, c = tap_of(p)
            return pad[c, xr, 2 - b : 2 - b + LY].reshape(LY * LZ, C)

        cells = LY * LZ
        lhs = xt[:, :cells] if k == 0 else xt[:, CELLS - cells :]
        add_side(lhs, [p for p in range(27) if p % 9 // 3 == (2 if k == 0 else 0)], view_x)
    quads(0)
    def lay_out(side):
        edges = [zcorner[side, e].astype(f32) for e in range(2)]
        for i in range(10):
            plane[side, i, 8 : 8 + LY, :] = zhalo[side, i].astype(f32)
            for e, yr in ((0, 7), (1, 8 + LY)):
                if 0 < i < 9:
                    plane[side, i, yr : yr + 1, :] = edges[e][i - 1 : i]
                else:
                    plane[side, i, yr : yr + 1, :] = zdot[side, e, i // 9]
        for i in range(10):
            turned[1, i] = zhalo[side, i]
            for b in (0, 2):
                turned[b, i] = plane[side, i, 9 - b : 9 - b + LY, :].astype(bf16)

    def put_in(side):
        zr = 7 + 17 * side

        def put(i, _):
            full2[pl.ds(i * 18 * PITCH + zr, 18, stride=PITCH), :] = plane[side, i, 7 : 7 + 18, :]
            return 0

        lax.fori_loop(0, 10, put, 0)

    def view_z(p):
        a, b, _ = tap_of(p)
        return turned[b, 2 - a : 2 - a + LX].reshape(LX * LY, C)

    wide_wait(False)
    lay_out(early_side)
    add_side(xz[early_side], range(9, 18), view_z)
    quads(1)
    far = jnp.logical_or(gz == 3, gz == 4)

    halves = (slice(0, 14 * C), slice(14 * C, 27 * C))

    def slab(g, h):
        return w.at[pl.ds(pl.multiple_of(g * 16, 16), 16), halves[h]]

    def filter_rows():
        drain(part.at[pl.ds(0, 31)], wr.at[1])
        drain(raws.at[pl.ds(0, 3)], wr.at[0])
        total = part[0]
        for j in range(1, 32):
            total = total + part[j]
        mean = total[0:1] / FAN
        var = total[1:2] / FAN - mean * mean
        inv = lax.rsqrt(var + var_eps)
        norm[0:1, :] = mean
        norm[1:2, :] = var
        norm[2:3, :] = inv
        for t in range(27):
            for j in range(4):
                mine_raw[t, 4 * j : 4 * j + 4, :] = raws[j, t]
        mine_rows = pl.ds(pl.multiple_of(gx * 16, 16), 16)
        for p in range(27):
            a, b, c = TAPS[p]
            t = 9 * a + 3 * b + c
            w[mine_rows, p * C : (p + 1) * C] = ((mine_raw[t] - mean) * inv).astype(bf16)
        for t in range(27):
            mine_std[4 * t : 4 * t + 4, :] = (raw_ref[t] - mean) * inv
        for h in range(2):
            for step in (8, 1, 7):
                remote(slab(gx, h), slab(gx, h), wr.at[2 + h], chip_peer(step)).start()
        for h in range(2):
            remote(slab(gx, h), slab(gx, h), ours.at[h], partner).start()

    def finish():
        wide_wait(True)
        lay_out(late_side)
        late = jnp.concatenate([view_z(p) for p in range(18, 27)], axis=1)
        quads(2, jnp.dot(xz[late_side], late, preferred_element_type=f32))

    @pl.when(jnp.logical_not(far))
    def _():
        finish()

    spread_chunk(0)
    spread_chunk(1)

    @pl.when(far)
    def _():
        filter_rows()
        finish()

    spread_chunk(2)

    @pl.when(jnp.logical_not(far))
    def _():
        filter_rows()

    mean, var, inv = norm[0:1, :], norm[1:2, :], norm[2:3, :]

    def hand_on(h):
        drain(w.at[pl.ds(0, 48), halves[h]], wr.at[2 + h])
        for k in (1, 2, 3):
            g = at_gx[k][0]
            remote(slab(g, h), slab(g, h), ours.at[h], partner).start()

    def take_over(h):
        drain(w.at[pl.ds(0, 64), halves[h]], ours.at[h])
        for p in range(14 * h, 14 + 13 * h):
            wt[p * C : (p + 1) * C, :] = w[:, p * C : (p + 1) * C].T

    def input_grad(h, lo, hi):
        def one(i, _):
            views = []
            for a, b, c in TAPS[14 * h : 14 + 13 * h]:
                views.append(pad[c, pl.ds(2 * i + 2 - a, 2), 2 - b : 2 - b + LY].reshape(2 * LY * LZ, C))
            out = jnp.dot(jnp.concatenate(views, axis=1), wt[halves[h], :], preferred_element_type=f32)
            if h == 0:
                part_dx[i] = out
            else:
                dx_ref[pl.ds(2 * i, 2)] = (part_dx[i] + out).astype(bf16).reshape(2, LY, LZ, C)
            return 0

        lax.fori_loop(lo, hi, one, 0)

    put_in(0)
    put_in(1)
    lax.fori_loop(0, 10, shift, 0)
    hand_on(0)
    drain(r1, got.at[1])
    for q in range(7):
        acc = own[q, mine] + precv[q, mine].astype(f32)
        for k in range(15):
            acc = acc + r1[k, q].astype(f32)
        red[q * 16 : (q + 1) * 16, :] = acc
    for j in range(4):
        for n, start in enumerate((0, 72 - 36 * z_hi, 36 + 36 * z_hi)):
            comp[j, 9 * n : 9 * n + 9, :] = red[pl.ds(start + j, 9, stride=4), :]
        comp[j, 27:32, :] = jnp.zeros((5, C), f32)
        rows[j] = comp[j].astype(bf16)
    r2[z] = rows[z_lo]

    for k in (4, 3, 5, 2, 6, 1, 7):
        remote(rows.at[spots[k][0]], r2.at[z], got.at[2], z_peer(k)).start()

    take_over(0)
    input_grad(0, 0, 4)
    hand_on(1)
    drain(r2.at[pl.ds(0, 7)], got.at[2])
    acc = r2[0].astype(f32)
    for j in range(1, 8):
        acc = acc + r2[j].astype(f32)
    gath[x] = acc

    for k in (2, 1, 3):
        remote(gath.at[x], gath.at[x], got.at[3], x_peer(k)).start()
    take_over(1)
    input_grad(1, 0, 2)

    drain(gath.at[pl.ds(0, 3)], got.at[3])
    for r in range(4):
        for n, c in enumerate((1, 0, 2)):
            nat[pl.ds(4 * c + r, 9, stride=12), :] = gath[r, n * 9 : n * 9 + 9, :]
    g = nat[0:108, :]
    std = mine_std[0:108, :]
    here = gx * 4 + gy
    stat[here, 0:1, :] = jnp.sum(g, axis=0, keepdims=True)
    stat[here, 1:2, :] = jnp.sum(g * std, axis=0, keepdims=True)
    stat[here, 2:3, :] = jnp.sum(g * g, axis=0, keepdims=True)
    stat[here, 3:4, :] = jnp.zeros((1, C), f32)

    def send_stat(device):
        remote(stat.at[here], stat.at[here], got.at[4], device).start()

    to_plane(send_stat)
    input_grad(1, 2, 4)
    drain(stat.at[pl.ds(0, 31)], got.at[4])
    total = stat[0]
    for j in range(1, 32):
        total = total + stat[j]
    sum_grad, sum_cross, sum_square = total[0:1], total[1:2], total[2:3]
    mean_grad = sum_grad / FAN
    mean_cross = sum_cross / FAN
    per_output = sum_square - 2.0 * mean_grad * sum_grad - 2.0 * mean_cross * sum_cross
    per_output = (
        per_output + FAN * mean_grad * mean_grad + FAN * mean_cross * mean_cross * var / (var + var_eps)
    )
    square_sum = jnp.sum(inv * inv * per_output, axis=1, keepdims=True)
    scale = jnp.minimum(1.0, clip_norm * lax.rsqrt(square_sum + norm_eps))
    factor = inv * scale
    for t in range(27):
        g = nat[4 * t : 4 * t + 4, :]
        dw_ref[t] = factor * (g - mean_grad - mine_std[4 * t : 4 * t + 4, :] * mean_cross)

    always = (3 * 27 * 4 * C + 31 * 2 * C + 31 * 4 * C + 3 * 32 * C) * 4 + (
        7 * 16 * 27 * C + 7 * 256 * C + 15 * 112 * C + 7 * 32 * C
    ) * 2
    for nz in (1, 2):

        @pl.when(near_z == nz)
        def _(nz=nz):
            by_neighbours(
                lambda nx, ny: flat_rows(nx, ny) + nz * wide_rows(nx, ny) + always // (4 * C), sent.at[0]
            )


def hand_over(dx_in, dw_in, dx_out, dw_out, sems):
    copies = [
        pltpu.make_async_copy(a, b, sems.at[n]) for n, (a, b) in enumerate(((dx_in, dx_out), (dw_in, dw_out)))
    ]
    for copy in copies:
        copy.start()
    for copy in copies:
        copy.wait()


def on_device(raw_weight, inputs, cotangent):
    dma = pltpu.SemaphoreType.DMA
    vmem = pltpu.VMEM
    dx, dw = pl.pallas_call(
        body,
        out_shape=(
            pltpu.VMEM(inputs.shape, bf16),
            pltpu.VMEM((27, 4, C), f32),
        ),
        in_specs=[pl.BlockSpec(memory_space=pltpu.HBM)] * 3,
        out_specs=[pl.BlockSpec(memory_space=pltpu.VMEM)] * 2,
        scratch_shapes=[
            vmem((27, 4, C), f32),
            vmem((LX, LY, LZ, C), bf16),
            vmem((LX, LY, LZ, C), bf16),
            vmem((11, 18, PITCH, C), f32),
            vmem((3, 10, 18, LZ, C), bf16),
            vmem((2, LX, LY, C), bf16),
            vmem((2, 2, 8, C), bf16),
            vmem((2, 2, 2, 1, C), f32),
            vmem((2, 10, LY, C), bf16),
            vmem((2, 2, 8, C), bf16),
            vmem((2, 2, 2, 1, C), f32),
            vmem((2, 10, 32, C), f32),
            vmem((3, 10, LY, C), bf16),
            vmem((CELLS + LZ, C), f32),
            vmem((C, CELLS), bf16),
            vmem((2, C, C), bf16),
            vmem((2, C, C), bf16),
            vmem((28, C, C), f32),
            vmem((2, LY, LZ, C), bf16),
            vmem((2, LX, LZ, C), bf16),
            vmem((2, 2, LZ, C), bf16),
            vmem((4, 27, 4, C), f32),
            vmem((27, 16, C), f32),
            vmem((32, 2, C), f32),
            vmem((8, C), f32),
            vmem((C, 27 * C), bf16),
            vmem((27 * C, C), bf16),
            vmem((LX // 2, 2 * LY * LZ, C), f32),
            vmem((7, 16, 16, C), f32),
            vmem((7, 16, 16, C), bf16),
            vmem((7, 16, 16, C), bf16),
            vmem((16, 7, 16, C), bf16),
            vmem((15, 7, 16, C), bf16),
            vmem((112, C), f32),
            vmem((4, 32, C), f32),
            vmem((8, 32, C), bf16),
            vmem((4, 32, C), bf16),
            vmem((4, 32, C), f32),
            vmem((120, C), f32),
            vmem((112, C), f32),
            vmem((32, 4, C), f32),
            dma((3,)),
            dma((3,)),
            dma((4,)),
            dma((3,)),
            dma((2,)),
            dma((5,)),
            dma((1,)),
        ],
        compiler_params=pltpu.CompilerParams(
            collective_id=0, has_side_effects=True, vmem_limit_bytes=40 * 1024 * 1024
        ),
    )(*[pltpu.with_memory_space_constraint(a, pltpu.HBM) for a in (jnp.swapaxes(raw_weight, 0, 1), inputs, cotangent)])
    dx, dw = pl.pallas_call(
        hand_over,
        out_shape=(jax.ShapeDtypeStruct(dx.shape, bf16), jax.ShapeDtypeStruct(dw.shape, f32)),
        in_specs=[pl.BlockSpec(memory_space=pltpu.VMEM)] * 2,
        out_specs=[pl.BlockSpec(memory_space=pl.ANY)] * 2,
        scratch_shapes=[dma((2,))],
    )(*[pltpu.with_memory_space_constraint(a, pltpu.VMEM) for a in (dx, dw)])
    return dx, jnp.swapaxes(dw, 0, 1)


def solution(mesh):
    in_specs = (P(("gx", "gy"), None, None), P("gx", "gy", "gz", None), P("gx", "gy", "gz", None))
    out_specs = (P("gx", "gy", "gz", None), P(("gx", "gy"), None, None))
    return jax.shard_map(
        on_device, mesh=mesh, in_specs=in_specs, out_specs=out_specs, check_vma=False
    )
```

```python
import functools

import jax
import jax.numpy as jnp
from jax import lax
from jax.experimental import pallas as pl
from jax.experimental.pallas import tpu as pltpu
from jax.sharding import PartitionSpec as P

var_eps = 1e-05
norm_eps = 1e-06
clip_norm = 600.0

f32 = jnp.float32
bf16 = jnp.bfloat16
MESH = pl.DeviceIdType.MESH

C = 128
LX, LY, LZ = 8, 16, 16
CELLS = LX * LY * LZ
PITCH = 32
FAN = 27 * C

TAPS = [(t // 9, t // 3 % 3, t % 3) for t in range(27)]
CHUNKS = ((0, 2), (2, 4), (4, 7))
DIRECTIONS = [
    (dx, dy, dz)
    for dz in (-1, 1, 0)
    for dx in (0, -1, 1)
    for dy in (0, -1, 1)
    if (dx, dy, dz) != (0, 0, 0)
]


def body(raw_hbm, x_hbm, cot_hbm, dx_ref, dw_ref, raw_ref, x_ref, cot_ref,
         full, pad, zface, zedge, zpoint, zhalo, zcorner, zdot, plane, turned, xf, xt, xy, xz, grad, land_x, land_y, land_c,
         raws, mine_raw, part, norm, w, wt, part_dx, own, psend, precv, spread, r1, red, comp, r2, rows, gath, nat, mine_std, stat,
         ls, hr, wr, dr, ours, got, sent):
    gx, gy, gz = lax.axis_index("gx"), lax.axis_index("gy"), lax.axis_index("gz")
    def div(a, n):
        return lax.div(a, jnp.int32(n))

    def mod(a, n):
        return lax.rem(a, jnp.int32(n))

    z_lo, core = div(gx, 2), mod(gx, 2)
    z_hi, x = div(gz, 4), mod(gz, 4)
    z = z_hi * 4 + z_lo
    mine = gy * 4 + x
    early_tap, late_tap = 2 - 2 * z_hi, 2 * z_hi
    early_side, late_side = z_hi, 1 - z_hi
    full2 = full.reshape(11 * 18 * PITCH, C)

    def dev(a, b, c):
        return (a, b, c)

    def ring(step):
        zz = mod(z + step, 8)
        return mod(zz, 4), div(zz, 4)

    spots = [ring(step) for step in range(8)] + [ring(2 + 4 * core), (mod(z_lo + 2, 4), z_hi)]
    at_gz = [hi * 4 + x for _, hi in spots]
    at_gx = [[lo * 2 + core, lo * 2 + 1 - core] for lo, _ in spots]
    at_gy = [gy] + [mod(gy + k, 4) for k in range(1, 4)]
    at_x = [x] + [mod(x + k, 4) for k in range(1, 4)]
    x_gz = [gz] + [z_hi * 4 + at_x[k] for k in range(1, 4)]

    def chip_peer(step):
        return dev(at_gx[step][0], gy, at_gz[step])

    def gy_peer(k):
        return dev(gx, at_gy[k], gz)

    def x_peer(k):
        return dev(gx, gy, x_gz[k])

    def xy_peer(k):
        return dev(gx, at_gy[k // 4], x_gz[k % 4])

    z_peer = chip_peer
    def plane_peer(k, step):
        return dev(at_gx[step][k // 4], at_gy[k % 4], at_gz[step])

    def to_plane(send):
        for step in (9, 1, 7, 0):
            for k in range(1 if step == 0 else 0, 8):
                send(plane_peer(k, step))

    partner = dev(gx + 1 - 2 * core, gy, gz)

    def remote(src, dst, recv, device):
        return pltpu.make_async_remote_copy(
            src_ref=src, dst_ref=dst, send_sem=sent.at[0], recv_sem=recv, device_id=device, device_id_type=MESH
        )

    def rows_wait(n, sem):
        view = full2.at[pl.ds(0, n)]
        pltpu.make_async_copy(view, view, sem).wait()

    def drain(ref, sem):
        pltpu.make_async_copy(ref, ref, sem).wait()

    def exists(axis_index, last, step):
        if step == 0:
            return None
        return axis_index > 0 if step < 0 else axis_index < last

    def count(axis_index, last):
        return (axis_index > 0).astype(jnp.int32) + (axis_index < last).astype(jnp.int32)

    def present(d):
        tests = [exists(gx, 7, d[0]), exists(gy, 3, d[1]), exists(gz, 7, d[2])]
        tests = [t for t in tests if t is not None]
        out = tests[0]
        for t in tests[1:]:
            out = jnp.logical_and(out, t)
        return out

    loads = [
        pltpu.make_async_copy(a, b, ls.at[n])
        for n, (a, b) in enumerate(((cot_hbm, cot_ref), (raw_hbm, raw_ref), (x_hbm, x_ref)))
    ]
    for load in loads:
        load.start()

    barrier = pltpu.get_barrier_semaphore()

    def greet(device):
        pl.semaphore_signal(barrier, inc=1, device_id=device, device_id_type=MESH)

    wide = [d for d in DIRECTIONS if d[2] != 0]
    greeted = jnp.int32(0)
    for d in wide:
        there = present(d)

        @pl.when(there)
        def _(d=d):
            greet(dev(gx + d[0], gy + d[1], gz + d[2]))

        greeted = greeted + there.astype(jnp.int32)
    greet(z_peer(2))
    greet(z_peer(6))
    for k in (10, 11, 9, 6, 14, 5, 7, 13, 15, 1, 2, 3):
        greet(xy_peer(k))
    to_plane(greet)

    loads[0].wait()

    def fill(i, _):
        slab = cot_ref[i]
        pad[1, i + 1, 1 : LY + 1] = slab
        full[i + 1, 1 : LY + 1, 8 : 8 + LZ, :] = slab.astype(f32)
        return 0

    lax.fori_loop(0, LX, fill, 0)

    def faces(i, _):
        for s, zr in ((0, 8), (1, 8 + LZ - 1)):
            zface[s, i] = full2[pl.ds(((i + 1) * 18 + 1) * PITCH + zr, LY, stride=PITCH), :].astype(bf16)
        return 0

    lax.fori_loop(0, LX, faces, 0)
    for s, zr in ((0, 8), (1, 8 + LZ - 1)):
        for e, yr in ((0, 1), (1, LY)):
            for i in range(LX):
                at = ((i + 1) * 18 + yr) * PITCH + zr
                plane[s, e, i : i + 1, :] = full2[at : at + 1, :]
            zedge[s, e] = plane[s, e, 0:LX, :].astype(bf16)
            zpoint[s, e, 0] = plane[s, e, 0:1, :]
            zpoint[s, e, 1] = plane[s, e, LX - 1 : LX, :]
    loads[1].wait()
    raws[gy] = raw_ref[...]
    first = jnp.zeros((4, C), f32)
    second = jnp.zeros((4, C), f32)
    for t in range(27):
        v = raw_ref[t]
        first = first + v
        second = second + v * v
    part[gx * 4 + gy, 0:1, :] = jnp.sum(first, axis=0, keepdims=True)
    part[gx * 4 + gy, 1:2, :] = jnp.sum(second, axis=0, keepdims=True)

    pl.semaphore_wait(barrier, greeted + (2 + 12 + 31))

    def halo_copy(d):
        dx, dy, dz = d
        xs, xd = (None, None) if dx == 0 else ((0, 1) if dx < 0 else (LX - 1, 0))
        ys, yd = (None, None) if dy == 0 else ((0, 1) if dy < 0 else (LY - 1, 0))
        if dz == 0:
            if dy == 0:
                src, dst = cot_ref.at[xs], land_x.at[xd]
            elif dx == 0:
                src, dst = cot_ref.at[:, ys], land_y.at[yd]
            else:
                src, dst = cot_ref.at[xs, ys], land_c.at[xd, yd]
        else:
            s = 0 if dz < 0 else 1
            r = 1 - s
            if dy == 0:
                if dx == 0:
                    src, dst = zface.at[s], zhalo.at[r, pl.ds(1, LX)]
                else:
                    src, dst = zface.at[s, xs], zhalo.at[r, 9 * xd]
            else:
                e = 0 if dy < 0 else 1
                if dx == 0:
                    src, dst = zedge.at[s, e], zcorner.at[r, 1 - e]
                elif dx < 0:
                    src, dst = zpoint.at[s, e, 0], zdot.at[r, 1 - e, 1]
                else:
                    src, dst = zpoint.at[s, e, 1], zdot.at[r, 1 - e, 0]
        return remote(src, dst, hr.at[0 if dz == 0 else (2 if dz < 0 else 1)], dev(gx + dx, gy + dy, gz + dz))

    def send_part(device):
        here = part.at[gx * 4 + gy]
        remote(here, here, wr.at[1], device).start()

    busy = jnp.logical_or(gz == 3, gz == 4)

    def large(d):
        return d[1] == 0 and d[2] == 0

    for d in DIRECTIONS:
        there = present(d)
        if large(d):
            there = jnp.logical_and(there, jnp.logical_not(busy))

        @pl.when(there)
        def _(d=d):
            halo_copy(d).start()

    near_x, near_y, near_z = count(gx, 7), count(gy, 3), count(gz, 7)

    def flat_rows(nx, ny):
        return 128 * nx + 64 * ny + 8 * nx * ny

    def wide_rows(nx, ny):
        return 64 + 8 * nx + 4 * ny + nx * ny

    def by_neighbours(rows, sem):
        for nx in (1, 2):
            for ny in (1, 2):

                @pl.when(jnp.logical_and(near_x == nx, near_y == ny))
                def _(nx=nx, ny=ny):
                    rows_wait(rows(nx, ny), sem)

    def wide_wait(late):
        for half in (0, 1):
            there = z_hi == half
            if not late:
                there = jnp.logical_and(there, near_z == 2)

            @pl.when(there)
            def _(half=half):
                by_neighbours(wide_rows, hr.at[1 + (1 - half if late else half)])

    for k in (2, 1, 3):
        remote(raw_ref, raws.at[gy], wr.at[0], gy_peer(k)).start()

    tile = jnp.zeros((LZ, C), bf16)

    for c in range(3):
        for i in (0, 9):
            for j in range(18):
                pad[c, i, j] = tile
        for i in range(1, 9):
            pad[c, i, 0] = tile
            pad[c, i, 17] = tile

    for k, x_there in ((0, gx > 0), (1, gx < 7)):

        @pl.when(jnp.logical_not(x_there))
        def _(k=k):
            for j in range(LY):
                land_x[k, j] = tile

        for e, y_there in ((0, gy > 0), (1, gy < 3)):

            @pl.when(jnp.logical_not(jnp.logical_and(x_there, y_there)))
            def _(k=k, e=e):
                land_c[k, e] = tile

    for e, y_there in ((0, gy > 0), (1, gy < 3)):

        @pl.when(jnp.logical_not(y_there))
        def _(e=e):
            for i in range(LX):
                land_y[e, i] = tile

    for r, z_there in ((0, gz > 0), (1, gz < 7)):

        @pl.when(jnp.logical_not(z_there))
        def _(r=r):
            for i in range(10):
                zhalo[r, i] = tile

        for k, x_there in ((0, gx > 0), (1, gx < 7)):

            @pl.when(jnp.logical_and(z_there, jnp.logical_not(x_there)))
            def _(r=r, k=k):
                zhalo[r, 9 * k] = tile

        for e, y_there in ((0, gy > 0), (1, gy < 3)):
            both = jnp.logical_and(z_there, y_there)

            @pl.when(jnp.logical_not(both))
            def _(r=r, e=e):
                zcorner[r, e] = jnp.zeros((8, C), bf16)

            for k, x_there in ((0, gx > 0), (1, gx < 7)):

                @pl.when(jnp.logical_not(jnp.logical_and(both, x_there)))
                def _(r=r, e=e, k=k):
                    zdot[r, e, k] = jnp.zeros((1, C), f32)

    for i in range(10):
        for zr in (7, 8 + LZ):
            full2[pl.ds(i * 18 * PITCH + zr, 18, stride=PITCH), :] = jnp.zeros((18, C), f32)

    def shift(i, _):
        pad[0, i] = full[i, :, 9 : 9 + LZ, :].astype(bf16)
        pad[2, i] = full[i, :, 7 : 7 + LZ, :].astype(bf16)
        return 0

    def shift_inside(i, _):
        inside = slice(1, LY + 1)
        pad[0, i, inside] = full[i, inside, 9 : 9 + LZ, :].astype(bf16)
        pad[2, i, inside] = full[i, inside, 7 : 7 + LZ, :].astype(bf16)
        return 0

    lax.fori_loop(1, LX + 1, shift_inside, 0)
    loads[2].wait()
    m = lax.broadcasted_iota(jnp.int32, (C, C), 0)
    col = lax.broadcasted_iota(jnp.int32, (C, C), 1)
    want = (m % 4) * 32 + (m // 4 + 16 * core) % 32
    order = jnp.where(col == want, 1.0, 0.0).astype(bf16)
    for j in range(4):
        xt[:, j * 512 : (j + 1) * 512] = lax.dot_general(
            order,
            x_ref[2 * j : 2 * j + 2].reshape(512, C),
            (((1,), (1,)), ((), ())),
            preferred_element_type=f32,
        ).astype(bf16)

    for d in DIRECTIONS:
        if large(d):

            @pl.when(jnp.logical_and(present(d), busy))
            def _(d=d):
                halo_copy(d).start()

    to_plane(send_part)

    def widen(i, _):
        xf[pl.ds(pl.multiple_of(i * LY * LZ, LY * LZ), LY * LZ), :] = x_ref[i].reshape(LY * LZ, C).astype(f32)
        return 0

    lax.fori_loop(0, LX, widen, 0)
    def by_channel(cells):
        return lax.dot_general(order, cells, (((1,), (1,)), ((), ())), preferred_element_type=f32).astype(bf16)

    for n, e in ((0, 0), (1, LZ - 1)):
        xy[n] = by_channel(x_ref[:, e].reshape(LX * LZ, C))
        xz[n] = by_channel(xf[pl.ds(e, LX * LY, stride=LZ), :].astype(bf16))

    def tap_of(p):
        return p % 9 // 3, p % 3, (1, early_tap, late_tap)[p // 9]

    for p in range(0, 27, 2):
        views = []
        for t in range(p, min(p + 2, 27)):
            a, b, c = tap_of(t)
            views.append(pad[c, 2 - a : 2 - a + LX, 2 - b : 2 - b + LY].reshape(CELLS, C))
        v = jnp.concatenate(views, axis=1) if len(views) == 2 else views[0]
        o = jnp.dot(xt[...], v, preferred_element_type=f32)
        for n in range(len(views)):
            grad[p + n] = o[:, n * C : (n + 1) * C]
    grad[27] = jnp.zeros((C, C), f32)

    def add_side(lhs, taps, view):
        o = jnp.dot(lhs, jnp.concatenate([view(p) for p in taps], axis=1), preferred_element_type=f32)
        for n, p in enumerate(taps):
            grad[p] += o[:, n * C : (n + 1) * C]

    def quad(q, late=None):
        outs = [grad[p] for p in range(4 * q, 4 * q + 4)]
        if late is not None:
            for n, p in enumerate(range(4 * q, 4 * q + 4)):
                if 18 <= p < 27:
                    outs[n] = outs[n] + late[:, (p - 18) * C : (p - 17) * C]
        low = lax.broadcasted_iota(jnp.int32, (16, 8, C), 1) < 4
        pieces = [[], []]
        for h in range(2):
            one = outs[2 * h].reshape(16, 8, C)
            two = outs[2 * h + 1].reshape(16, 8, C)
            pieces[0].append(jnp.where(low, one, pltpu.roll(two, 4, 1)))
            pieces[1].append(jnp.where(low, pltpu.roll(one, 4, 1), two))
        for e in range(2):
            t = jnp.concatenate(pieces[e], axis=1)
            for j in range(8):
                own[q, 2 * j + e] = t[j]
                psend[q, 2 * j + e] = t[8 + j].astype(bf16)

    def quads(n, late=None):
        lo, hi = CHUNKS[n]
        step = 1 if n == 2 else hi - lo
        for q in range(lo, hi):
            quad(q, late)
            if (q - lo) % step == step - 1:
                some = pl.ds(q - step + 1, step)
                remote(psend.at[some], precv.at[some], dr.at[q - 2 if n == 2 else n], partner).start()

    def spread_chunk(n):
        lo, hi = CHUNKS[n]
        if n < 2:
            drain(precv.at[pl.ds(lo, hi - lo)], dr.at[n])
        for q in range(lo, hi):
            if n == 2:
                drain(precv.at[pl.ds(q, 1)], dr.at[q - 2])
            spread[:, q] = (own[q] + precv[q].astype(f32)).astype(bf16)

        for k in (10, 11, 9, 6, 14, 2, 8, 5, 7, 13, 15, 1, 3, 4, 12):
            remote(
                spread.at[at_gy[k // 4] * 4 + at_x[k % 4], pl.ds(lo, hi - lo)],
                r1.at[k - 1, pl.ds(lo, hi - lo)],
                got.at[1],
                xy_peer(k),
            ).start()

    by_neighbours(flat_rows, hr.at[0])
    for e, yr in ((0, 0), (1, LY + 1)):
        face = land_y[e]
        pad[1, 1 : LX + 1, yr] = face
        full[1 : LX + 1, yr, 8 : 8 + LZ, :] = face.astype(f32)
        pad[0, 1 : LX + 1, yr] = full[1 : LX + 1, yr, 9 : 9 + LZ, :].astype(bf16)
        pad[2, 1 : LX + 1, yr] = full[1 : LX + 1, yr, 7 : 7 + LZ, :].astype(bf16)

        def view_y(p, yr=yr):
            a, _, c = tap_of(p)
            return pad[c, 2 - a : 2 - a + LX, yr].reshape(LX * LZ, C)

        add_side(xy[e], [p for p in range(27) if p % 3 == (2 if e == 0 else 0)], view_y)
    for k, xr in ((0, 0), (1, LX + 1)):
        pad[1, xr, 1 : LY + 1] = land_x[k]
        full[xr, 1 : LY + 1, 8 : 8 + LZ, :] = land_x[k].astype(f32)
        for e, yr in ((0, 0), (1, LY + 1)):
            pad[1, xr, yr] = land_c[k, e]
            full[xr, yr, 8 : 8 + LZ, :] = land_c[k, e].astype(f32)
        shift(xr, 0)

        def view_x(p, xr=xr):
            _, b, c = tap_of(p)
            return pad[c, xr, 2 - b : 2 - b + LY].reshape(LY * LZ, C)

        cells = LY * LZ
        lhs = xt[:, :cells] if k == 0 else xt[:, CELLS - cells :]
        add_side(lhs, [p for p in range(27) if p % 9 // 3 == (2 if k == 0 else 0)], view_x)
    quads(0)
    def lay_out(side):
        edges = [zcorner[side, e].astype(f32) for e in range(2)]
        for i in range(10):
            plane[side, i, 8 : 8 + LY, :] = zhalo[side, i].astype(f32)
            for e, yr in ((0, 7), (1, 8 + LY)):
                if 0 < i < 9:
                    plane[side, i, yr : yr + 1, :] = edges[e][i - 1 : i]
                else:
                    plane[side, i, yr : yr + 1, :] = zdot[side, e, i // 9]
        for i in range(10):
            turned[1, i] = zhalo[side, i]
            for b in (0, 2):
                turned[b, i] = plane[side, i, 9 - b : 9 - b + LY, :].astype(bf16)

    def put_in(side):
        zr = 7 + 17 * side

        def put(i, _):
            full2[pl.ds(i * 18 * PITCH + zr, 18, stride=PITCH), :] = plane[side, i, 7 : 7 + 18, :]
            return 0

        lax.fori_loop(0, 10, put, 0)

    def view_z(p):
        a, b, _ = tap_of(p)
        return turned[b, 2 - a : 2 - a + LX].reshape(LX * LY, C)

    wide_wait(False)
    lay_out(early_side)
    add_side(xz[early_side], range(9, 18), view_z)
    quads(1)
    far = jnp.logical_or(gz == 3, gz == 4)

    halves = (slice(0, 14 * C), slice(14 * C, 27 * C))

    def slab(g, h):
        return w.at[pl.ds(pl.multiple_of(g * 16, 16), 16), halves[h]]

    def filter_rows():
        drain(part.at[pl.ds(0, 31)], wr.at[1])
        drain(raws.at[pl.ds(0, 3)], wr.at[0])
        total = part[0]
        for j in range(1, 32):
            total = total + part[j]
        mean = total[0:1] / FAN
        var = total[1:2] / FAN - mean * mean
        inv = lax.rsqrt(var + var_eps)
        norm[0:1, :] = mean
        norm[1:2, :] = var
        norm[2:3, :] = inv
        for t in range(27):
            for j in range(4):
                mine_raw[t, 4 * j : 4 * j + 4, :] = raws[j, t]
        mine_rows = pl.ds(pl.multiple_of(gx * 16, 16), 16)
        for p in range(27):
            a, b, c = TAPS[p]
            t = 9 * a + 3 * b + c
            w[mine_rows, p * C : (p + 1) * C] = ((mine_raw[t] - mean) * inv).astype(bf16)
        for t in range(27):
            mine_std[4 * t : 4 * t + 4, :] = (raw_ref[t] - mean) * inv
        for h in range(2):
            for step in (8, 1, 7):
                remote(slab(gx, h), slab(gx, h), wr.at[2 + h], chip_peer(step)).start()
        for h in range(2):
            remote(slab(gx, h), slab(gx, h), ours.at[h], partner).start()

    def finish():
        wide_wait(True)
        lay_out(late_side)
        late = jnp.concatenate([view_z(p) for p in range(18, 27)], axis=1)
        quads(2, jnp.dot(xz[late_side], late, preferred_element_type=f32))

    @pl.when(jnp.logical_not(far))
    def _():
        finish()

    spread_chunk(0)
    spread_chunk(1)

    @pl.when(far)
    def _():
        filter_rows()
        finish()

    spread_chunk(2)

    @pl.when(jnp.logical_not(far))
    def _():
        filter_rows()

    mean, var, inv = norm[0:1, :], norm[1:2, :], norm[2:3, :]

    def hand_on(h):
        drain(w.at[pl.ds(0, 48), halves[h]], wr.at[2 + h])
        for k in (1, 2, 3):
            g = at_gx[k][0]
            remote(slab(g, h), slab(g, h), ours.at[h], partner).start()

    def take_over(h):
        drain(w.at[pl.ds(0, 64), halves[h]], ours.at[h])
        for p in range(14 * h, 14 + 13 * h):
            wt[p * C : (p + 1) * C, :] = w[:, p * C : (p + 1) * C].T

    def input_grad(h, lo, hi):
        def one(i, _):
            views = []
            for a, b, c in TAPS[14 * h : 14 + 13 * h]:
                views.append(pad[c, pl.ds(2 * i + 2 - a, 2), 2 - b : 2 - b + LY].reshape(2 * LY * LZ, C))
            out = jnp.dot(jnp.concatenate(views, axis=1), wt[halves[h], :], preferred_element_type=f32)
            if h == 0:
                part_dx[i] = out
            else:
                dx_ref[pl.ds(2 * i, 2)] = (part_dx[i] + out).astype(bf16).reshape(2, LY, LZ, C)
            return 0

        lax.fori_loop(lo, hi, one, 0)

    put_in(0)
    put_in(1)
    lax.fori_loop(0, 10, shift, 0)
    hand_on(0)
    drain(r1, got.at[1])
    for q in range(7):
        acc = own[q, mine] + precv[q, mine].astype(f32)
        for k in range(15):
            acc = acc + r1[k, q].astype(f32)
        red[q * 16 : (q + 1) * 16, :] = acc
    for j in range(4):
        for n, start in enumerate((0, 72 - 36 * z_hi, 36 + 36 * z_hi)):
            comp[j, 9 * n : 9 * n + 9, :] = red[pl.ds(start + j, 9, stride=4), :]
        comp[j, 27:32, :] = jnp.zeros((5, C), f32)
        rows[j] = comp[j].astype(bf16)
    r2[z] = rows[z_lo]

    for k in (4, 3, 5, 2, 6, 1, 7):
        remote(rows.at[spots[k][0]], r2.at[z], got.at[2], z_peer(k)).start()

    take_over(0)
    input_grad(0, 0, 4)
    hand_on(1)
    drain(r2.at[pl.ds(0, 7)], got.at[2])
    acc = r2[0].astype(f32)
    for j in range(1, 8):
        acc = acc + r2[j].astype(f32)
    gath[x] = acc

    for k in (2, 1, 3):
        remote(gath.at[x], gath.at[x], got.at[3], x_peer(k)).start()
    take_over(1)
    input_grad(1, 0, 2)

    drain(gath.at[pl.ds(0, 3)], got.at[3])
    for r in range(4):
        for n, c in enumerate((1, 0, 2)):
            nat[pl.ds(4 * c + r, 9, stride=12), :] = gath[r, n * 9 : n * 9 + 9, :]
    g = nat[0:108, :]
    std = mine_std[0:108, :]
    here = gx * 4 + gy
    stat[here, 0:1, :] = jnp.sum(g, axis=0, keepdims=True)
    stat[here, 1:2, :] = jnp.sum(g * std, axis=0, keepdims=True)
    stat[here, 2:3, :] = jnp.sum(g * g, axis=0, keepdims=True)
    stat[here, 3:4, :] = jnp.zeros((1, C), f32)

    def send_stat(device):
        remote(stat.at[here], stat.at[here], got.at[4], device).start()

    to_plane(send_stat)
    input_grad(1, 2, 4)
    drain(stat.at[pl.ds(0, 31)], got.at[4])
    total = stat[0]
    for j in range(1, 32):
        total = total + stat[j]
    sum_grad, sum_cross, sum_square = total[0:1], total[1:2], total[2:3]
    mean_grad = sum_grad / FAN
    mean_cross = sum_cross / FAN
    per_output = sum_square - 2.0 * mean_grad * sum_grad - 2.0 * mean_cross * sum_cross
    per_output = (
        per_output + FAN * mean_grad * mean_grad + FAN * mean_cross * mean_cross * var / (var + var_eps)
    )
    square_sum = jnp.sum(inv * inv * per_output, axis=1, keepdims=True)
    scale = jnp.minimum(1.0, clip_norm * lax.rsqrt(square_sum + norm_eps))
    factor = inv * scale
    for t in range(27):
        g = nat[4 * t : 4 * t + 4, :]
        dw_ref[t] = factor * (g - mean_grad - mine_std[4 * t : 4 * t + 4, :] * mean_cross)

    always = (3 * 27 * 4 * C + 31 * 2 * C + 31 * 4 * C + 3 * 32 * C) * 4 + (
        7 * 16 * 27 * C + 7 * 256 * C + 15 * 112 * C + 7 * 32 * C
    ) * 2
    for nz in (1, 2):

        @pl.when(near_z == nz)
        def _(nz=nz):
            by_neighbours(
                lambda nx, ny: flat_rows(nx, ny) + nz * wide_rows(nx, ny) + always // (4 * C), sent.at[0]
            )


def hand_over(dx_in, dw_in, dx_out, dw_out, sems):
    copies = [
        pltpu.make_async_copy(a, b, sems.at[n]) for n, (a, b) in enumerate(((dx_in, dx_out), (dw_in, dw_out)))
    ]
    for copy in copies:
        copy.start()
    for copy in copies:
        copy.wait()


def on_device(raw_weight, inputs, cotangent):
    dma = pltpu.SemaphoreType.DMA
    vmem = pltpu.VMEM
    dx, dw = pl.pallas_call(
        body,
        out_shape=(
            pltpu.VMEM(inputs.shape, bf16),
            pltpu.VMEM((27, 4, C), f32),
        ),
        in_specs=[pl.BlockSpec(memory_space=pltpu.HBM)] * 3,
        out_specs=[pl.BlockSpec(memory_space=pltpu.VMEM)] * 2,
        scratch_shapes=[
            vmem((27, 4, C), f32),
            vmem((LX, LY, LZ, C), bf16),
            vmem((LX, LY, LZ, C), bf16),
            vmem((11, 18, PITCH, C), f32),
            vmem((3, 10, 18, LZ, C), bf16),
            vmem((2, LX, LY, C), bf16),
            vmem((2, 2, 8, C), bf16),
            vmem((2, 2, 2, 1, C), f32),
            vmem((2, 10, LY, C), bf16),
            vmem((2, 2, 8, C), bf16),
            vmem((2, 2, 2, 1, C), f32),
            vmem((2, 10, 32, C), f32),
            vmem((3, 10, LY, C), bf16),
            vmem((CELLS + LZ, C), f32),
            vmem((C, CELLS), bf16),
            vmem((2, C, C), bf16),
            vmem((2, C, C), bf16),
            vmem((28, C, C), f32),
            vmem((2, LY, LZ, C), bf16),
            vmem((2, LX, LZ, C), bf16),
            vmem((2, 2, LZ, C), bf16),
            vmem((4, 27, 4, C), f32),
            vmem((27, 16, C), f32),
            vmem((32, 2, C), f32),
            vmem((8, C), f32),
            vmem((C, 27 * C), bf16),
            vmem((27 * C, C), bf16),
            vmem((LX // 2, 2 * LY * LZ, C), f32),
            vmem((7, 16, 16, C), f32),
            vmem((7, 16, 16, C), bf16),
            vmem((7, 16, 16, C), bf16),
            vmem((16, 7, 16, C), bf16),
            vmem((15, 7, 16, C), bf16),
            vmem((112, C), f32),
            vmem((4, 32, C), f32),
            vmem((8, 32, C), bf16),
            vmem((4, 32, C), bf16),
            vmem((4, 32, C), f32),
            vmem((120, C), f32),
            vmem((112, C), f32),
            vmem((32, 4, C), f32),
            dma((3,)),
            dma((3,)),
            dma((4,)),
            dma((5,)),
            dma((2,)),
            dma((5,)),
            dma((1,)),
        ],
        compiler_params=pltpu.CompilerParams(
            collective_id=0, has_side_effects=True, vmem_limit_bytes=40 * 1024 * 1024
        ),
    )(*[pltpu.with_memory_space_constraint(a, pltpu.HBM) for a in (jnp.swapaxes(raw_weight, 0, 1), inputs, cotangent)])
    dx, dw = pl.pallas_call(
        hand_over,
        out_shape=(jax.ShapeDtypeStruct(dx.shape, bf16), jax.ShapeDtypeStruct(dw.shape, f32)),
        in_specs=[pl.BlockSpec(memory_space=pltpu.VMEM)] * 2,
        out_specs=[pl.BlockSpec(memory_space=pl.ANY)] * 2,
        scratch_shapes=[dma((2,))],
    )(*[pltpu.with_memory_space_constraint(a, pltpu.VMEM) for a in (dx, dw)])
    return dx, jnp.swapaxes(dw, 0, 1)


def solution(mesh):
    in_specs = (P(("gx", "gy"), None, None), P("gx", "gy", "gz", None), P("gx", "gy", "gz", None))
    out_specs = (P("gx", "gy", "gz", None), P(("gx", "gy"), None, None))
    return jax.shard_map(
        on_device, mesh=mesh, in_specs=in_specs, out_specs=out_specs, check_vma=False
    )
```
